256 devices in a mesh: mat: 4 (over z_lo), tile: 64 (over y, z_hi, x, core).
Axes of the slice: x: 4, y: 4, z: 8 (z_hi: 2, z_lo: 4; z = z_hi * 4 + z_lo), core: 2. Of those that a mesh axis runs over, the one named last changes fastest.
Arguments:
- volume: bfloat16 [4, 512, 64, 1024], P('mat', None, 'tile'), may hold values from -4 to 4
- system: bfloat16 [64, 1024, 32, 128], P('tile'), may hold values from 0 to 0.009521484
- geometry: int32 [64, 16], replicated, may hold values from 0 to 2
- attenuation: float32 [4, 64], replicated, may hold values from 0.05 to 0.5
- response: float32 [8, 64], replicated, may hold values from 0.002 to 0.06
- crosstalk: float32 [8], replicated, may hold values from 0.04 to 0.24
Outputs:
- counts: float32 [8, 512, 16, 512], P(None, ('mat', 'tile'))
The draws below stay inside these ranges and needn't reach their ends.
Inputs may be any that keep to these rules, and one draw needn't show every extreme that they name: A tile touches, in view v, exactly the 2 detector blocks geometry[t, v] to geometry[t, v] + 1.
All inputs are finite; a program needn't handle non-finite values.
Results may differ from the reference program's by a relative error of at most 0.0003.
Values may be sent and summed in bfloat16 or wider, within the bound.
A program may use at most 128 MiB of HBM per device.

```python
import math
import jax
import jax.numpy as jnp
from jax import lax

MATS = 4
TILE_VOX = 1024
VIEWS = 16
PIXELS = 512
PB = 128
TOUCH = 2
EBINS = 64
CBINS = 8
TILES = 64
SLICES = 512
PBLK = 4
KT = 32
RAYS = 8192


def place_ends(entries, rng, least, largest):
    shape = entries.shape
    place = [jax.random.randint(jax.random.fold_in(rng, axis), (), 0, shape[axis]) for axis in range(len(shape))]
    entries = entries.at[tuple(place)].set(least)
    longest = shape.index(max(shape))
    place[longest] = (place[longest] + 1) % shape[longest]
    return entries.at[tuple(place)].set(largest)


def level_of(stream_key, shape, cuts, low, high):
    level = 1.0
    for dim, shards_of in cuts:
        steps = jax.random.uniform(jax.random.fold_in(jax.random.fold_in(stream_key, 6), dim), (shards_of,), jnp.float32, low / len(cuts), high / len(cuts))
        level = level * jnp.repeat(jnp.exp(steps), shape[dim] // shards_of).reshape((-1,) + (1,) * (len(shape) - 1 - dim))
    return level


def noise(own_key, extent, width, bound, split=(), kind=jnp.bfloat16):
    values = jax.random.normal(own_key, extent, jnp.float32) * width
    if len(split) > 0:
        values = level_of(own_key, extent, split, -0.22, 0.18) * values
    return jnp.clip(values, min=-bound, max=bound).astype(kind)


def setup_inputs(seed: int = 0) -> dict:
    arg_keys = jax.random.split(jax.random.key(seed), 7)
    volume = noise(arg_keys[0], (MATS, SLICES, TILES, TILE_VOX), 1.0, 4.0, ((0, 4), (2, 64)))
    system = jnp.clip(0.009521484 * jax.random.uniform(arg_keys[1], (TILES, TILE_VOX, KT, PB), jnp.float32) ** level_of(arg_keys[1], (TILES, TILE_VOX, KT, PB), ((0, 64),), -0.2, 0.2), 0.0, 0.009521484).astype(jnp.bfloat16)
    geometry = place_ends(jax.random.randint(arg_keys[2], (TILES, VIEWS), 0, PBLK - TOUCH + 1), jax.random.fold_in(arg_keys[2], 1), 0, PBLK - TOUCH).astype(jnp.int32)
    attenuation = jnp.clip(jnp.exp(jax.random.uniform(arg_keys[3], (MATS, EBINS), jnp.float32, math.log(0.05), math.log(0.5))), 0.05, 0.5)
    response = jnp.clip(jnp.exp(jax.random.uniform(arg_keys[4], (CBINS, EBINS), jnp.float32, math.log(0.002), math.log(0.06))), 0.002, 0.06)
    crosstalk = jnp.clip(jax.random.uniform(arg_keys[5], (CBINS,), jnp.float32, 0.04, 0.24), 0.04, 0.24)
    return {"volume": volume, "system": system, "geometry": geometry, "attenuation": attenuation, "response": response, "crosstalk": crosstalk}


def reference(volume, system, geometry, attenuation, response, crosstalk):
    row_total = MATS * SLICES
    block_ids = jnp.arange(PBLK, dtype=jnp.int32)
    touch_ids = jnp.arange(TOUCH, dtype=jnp.int32)

    def one_tile(running, tile_index):
        columns = lax.dynamic_index_in_dim(volume, tile_index, 2, keepdims=False)
        columns = columns.reshape(row_total, TILE_VOX).astype(jnp.float32)
        matrix = lax.dynamic_index_in_dim(system, tile_index, 0, keepdims=False)
        matrix = matrix.reshape(TILE_VOX, KT * PB).astype(jnp.float32)
        partial_value = jnp.dot(columns, matrix, preferred_element_type=jnp.float32, precision=lax.Precision.HIGHEST)
        partial_value = partial_value.reshape(row_total, VIEWS, TOUCH, PB)
        first_block = lax.dynamic_index_in_dim(geometry, tile_index, 0, keepdims=False)
        placed = (first_block[:, None, None] + touch_ids[None, :, None] == block_ids[None, None, :]).astype(jnp.float32)
        expanded = jnp.einsum('rvjp,vjb->rvbp', partial_value, placed, precision=lax.Precision.HIGHEST)
        return (running + expanded, None)
    start_sums = jnp.zeros((row_total, VIEWS, PBLK, PB), jnp.float32)
    summed = lax.scan(one_tile, start_sums, jnp.arange(TILES, dtype=jnp.int32))[0]
    proj = summed.reshape(MATS, SLICES, RAYS).transpose(1, 0, 2)

    def one_row(integrals):
        exponent = jnp.dot(attenuation.T, integrals, preferred_element_type=jnp.float32, precision=lax.Precision.HIGHEST)
        return jnp.dot(response, jnp.exp(-exponent), preferred_element_type=jnp.float32, precision=lax.Precision.HIGHEST)
    detected = lax.map(one_row, proj).transpose(1, 0, 2)
    padded = jnp.pad(detected, ((0, 0), (1, 1), (0, 0)))
    leakage = crosstalk[:, None, None]
    counts = (1.0 - 2.0 * leakage) * detected + leakage * (padded[:, :-2] + padded[:, 2:])
    return counts.reshape(CBINS, SLICES, VIEWS, PIXELS)
```

```python
import functools

import jax
import jax.numpy as jnp
from jax import lax
from jax.experimental import pallas as pl
from jax.experimental.pallas import tpu as pltpu
from jax.sharding import PartitionSpec as P

MESH = pl.DeviceIdType.MESH
F32 = jnp.float32
BF16 = jnp.bfloat16
MATS = 4
VOX = 1024
VIEWS = 16
KT = 32
PB = 128
PIX = 512
EBINS = 64
CBINS = 8
SLICES = 512
HALF = SLICES // 2
PAIRS = VIEWS // 2
LOADS = 8
VOX_LOAD = VOX // LOADS
LAG_EXPAND = 1
LAG_RELAY = 2
LAG_OWNER = 3
LAG_CROSS = 4
LAG_DEPTH = 5
LAG_DETECT = 6


def kernel(
    vol_hbm, sys_hbm, geom, att, resp, leak,
    out,
    vol, rows, stage, weights,
    give, keep, take,
    ext, relay, arrive, owned, cross, fbuf,
    zsend, zrecv, proj, hsend, hrecv, obuf,
    load_sem, core_s, core_r, relay_s, relay_r, arrive_s, arrive_r,
    cross_s, cross_r, z_s, z_r, h_s, h_r,
):
    mat = lax.axis_index("mat")
    tile = lax.axis_index("tile")
    core = tile % 2
    x = (tile // 2) % 4
    zh = (tile // 8) % 2
    y = tile // 16
    z = zh * 4 + mat

    def tile_of(yy, zz, xx, cc):
        return ((yy * 2 + zz) * 4 + xx) * 2 + cc

    def x_peer(r):
        return (mat, tile_of(y, zh, (x + r) % 4, core))

    def y_peer(r):
        return (mat, tile_of((y + r) % 4, zh, x, core))

    def z_peer(r):
        zt = (z + r) % 8
        return (zt % 4, tile_of(y, zt // 4, x, core))

    partner = (mat, tile_of(y, zh, x, 1 - core))
    flat = mat * 64 + tile
    after = (flat + 1) % 256
    before = (flat + 255) % 256
    after = (after // 64, after % 64)
    before = (before // 64, before % 64)

    loads = [
        pltpu.make_async_copy(
            sys_hbm.at[pl.ds(n * VOX_LOAD, VOX_LOAD)],
            stage.at[pl.ds(n * VOX_LOAD, VOX_LOAD)],
            load_sem.at[n],
        )
        for n in range(LOADS)
    ]
    vol_load = pltpu.make_async_copy(vol_hbm, vol, load_sem.at[LOADS])
    vol_load.start()
    for load in loads:
        load.start()

    barrier = pltpu.get_barrier_semaphore()
    peers = [partner, after, before]
    peers += [x_peer(r) for r in (1, 2, 3)] + [y_peer(r) for r in (1, 2, 3)]
    peers += [z_peer(r) for r in range(1, 8)]
    for peer in peers:
        pl.semaphore_signal(barrier, inc=1, device_id=peer, device_id_type=MESH)

    r_id = lax.broadcasted_iota(jnp.int32, (SLICES, SLICES), 0)
    s_id = lax.broadcasted_iota(jnp.int32, (SLICES, SLICES), 1)
    r_core = (r_id >> 8) * (2 * core - 1) + (1 - core)
    r_y = ((r_id >> 6) + y) & 3
    r_x = ((r_id >> 4) + x) & 3
    r_mat = (r_id >> 2) & 3
    r_zh = (r_id >> 1) & 1
    want = r_mat * 128 + r_y * 32 + r_zh * 16 + r_x * 4 + r_core * 2 + (r_id & 1)
    order = jnp.where(s_id == want, 1.0, 0.0).astype(BF16)
    vol_load.wait()
    rows[...] = jnp.dot(order, vol[...], preferred_element_type=F32).astype(BF16)

    for n in range(LOADS):
        loads[n].wait()
        for h in range(VOX_LOAD // 64):
            u0 = n * VOX_LOAD + h * 64
            turned = jnp.swapaxes(stage[pl.ds(u0, 64)], 0, 1)
            for k in range(KT):
                weights[k // 2, pl.ds(u0, 64), pl.ds((k % 2) * PB, PB)] = turned[k]

    pl.semaphore_wait(barrier, len(peers))

    def send(src, dst, s, r, peer):
        copy = pltpu.make_async_remote_copy(
            src_ref=src, dst_ref=dst, send_sem=s, recv_sem=r, device_id=peer, device_id_type=MESH
        )
        return copy

    def give_copy(v):
        return send(give.at[v], take.at[v], core_s.at[v], core_r.at[v], partner)

    def chunk(v, u, r, half):
        if u == 0:
            return ext.at[v, pl.ds(half * 2, 2), r]
        return ext.at[v, r, pl.ds(half * 2, 2)]

    first_peer = (x_peer, y_peer)
    second_peer = (y_peer, x_peer)

    def far_copy(v, u, d):
        return send(
            chunk(v, u, 2, d), relay.at[v, d], relay_s.at[v, d], relay_r.at[v, d], first_peer[u]((1, 3)[d])
        )

    def near_copy(v, u, d, half):
        return send(
            chunk(v, u, (1, 3)[d], half),
            arrive.at[v, d, pl.ds(half * 2, 2)],
            arrive_s.at[v, d, half],
            arrive_r.at[v, d, half],
            first_peer[u]((1, 3)[d]),
        )

    def cross_copy(v, u, r):
        return send(
            owned.at[v, r], cross.at[v, r - 1], cross_s.at[v, r - 1], cross_r.at[v, r - 1], second_peer[u](r)
        )

    def z_copy(i, d):
        zt = (z + d) % 8
        q = (zt % 4) * 2 + zt // 4
        return send(
            zsend.at[i, pl.ds(pl.multiple_of(q * 16, 16), 16)],
            zrecv.at[i, z],
            z_s.at[i, d - 1],
            z_r.at[i, d - 1],
            z_peer(d),
        )

    def h_copy(i, d):
        return send(hsend.at[i, d], hrecv.at[i, d], h_s.at[i, d], h_r.at[i, d], (after, before)[d])

    def project(i):
        for u in range(2):
            v = i * 2 + u
            give[v] = jnp.dot(rows[pl.ds(0, HALF)], weights[v], preferred_element_type=F32)
            give_copy(v).start()
        for u in range(2):
            v = i * 2 + u
            keep[v] = jnp.dot(rows[pl.ds(HALF, HALF)], weights[v], preferred_element_type=F32)

    def expand(i):
        for u in range(2):
            v = i * 2 + u
            mine = geom[tile, v]
            theirs = geom[tile + 1 - 2 * core, v]
            give_copy(v).wait_recv()
            for n in range(HALF // 16):
                near = pl.ds(n * 16, 16)
                own0, own1 = keep[v, near, pl.ds(0, PB)], keep[v, near, pl.ds(PB, PB)]
                oth0, oth1 = take[v, near, pl.ds(0, PB)], take[v, near, pl.ds(PB, PB)]
                zero = jnp.zeros_like(own0)
                for b in range(4):
                    total = None
                    for first, part0, part1 in ((mine, own0, own1), (theirs, oth0, oth1)):
                        if b == 0:
                            term = jnp.where(first == 0, part0, zero)
                        elif b == 3:
                            term = jnp.where(first == 2, part1, zero)
                        else:
                            term = jnp.where(first == b, part0, jnp.where(first == b - 1, part1, zero))
                        total = term if total is None else total + term
                    ext[v, n // 4, n % 4, :, pl.ds(b * PB, PB)] = total
            far_copy(v, u, 0).start()
            far_copy(v, u, 1).start()
            near_copy(v, u, 0, 1).start()
            near_copy(v, u, 1, 0).start()

    def pass_on(i):
        for u in range(2):
            v = i * 2 + u
            for d in range(2):
                far_copy(v, u, d).wait_recv()
                target = chunk(v, u, (1, 3)[d], d)
                target[...] = target[...] + relay[v, d]
                near_copy(v, u, d, d).start()

    def gather(i):
        for u in range(2):
            v = i * 2 + u
            for d in range(2):
                for half in range(2):
                    near_copy(v, u, d, half).wait_recv()
            for n in range(4):
                mine = ext[v, n, 0] if u == 0 else ext[v, 0, n]
                owned[v, n] = mine + arrive[v, 0, n] + arrive[v, 1, n]
            for r in (2, 1, 3):
                cross_copy(v, u, r).start()

    def finish(i):
        for u in range(2):
            v = i * 2 + u
            for r in (1, 3, 2):
                cross_copy(v, u, r).wait_recv()
            for b in range(4):
                lanes = pl.ds(b * PB, PB)
                fbuf[u, b] = (owned[v, 0, :, lanes] + cross[v, 0, :, lanes]) + (
                    cross[v, 1, :, lanes] + cross[v, 2, :, lanes]
                )
            for b in range(4):
                for j in range(2):
                    part = fbuf[u, b, pl.ds(j, 8, stride=2), :]
                    zsend[i, pl.ds(u * 8 + j * 4 + b, 8, stride=16), :] = part
        for d in (4, 3, 5, 2, 6, 1, 7):
            z_copy(i, d).start()
        q = mat * 2 + zh
        zrecv[i, z] = zsend[i, pl.ds(pl.multiple_of(q * 16, 16), 16), :]

    sub = lax.broadcasted_iota(jnp.int32, (8, PB), 0)
    low = sub < 4

    def across(i):
        for d in range(1, 8):
            z_copy(i, d).wait_recv()
        for m in range(MATS):
            proj[i, m] = zrecv[i, m] + zrecv[i, 4 + m]
        for u in range(2):
            for p in range(2):
                even = proj[i, 2 * p, pl.ds(u * 8, 8), :]
                odd = proj[i, 2 * p + 1, pl.ds(u * 8, 8), :]
                hsend[i, 0, u, p] = jnp.where(low, pltpu.roll(even, 4, 0), odd)
                hsend[i, 1, u, p] = jnp.where(low, even, pltpu.roll(odd, 4, 0))
        h_copy(i, 0).start()
        h_copy(i, 1).start()

    inside = ((sub >= 4) | (flat > 0)) & ((sub < 4) | (flat < 255))

    def detect(i):
        for d in range(2):
            h_copy(i, d).wait_recv()
        for u in range(2):
            own = [proj[i, m, pl.ds(u * 8, 8), :] for m in range(MATS)]
            side = []
            for p in range(2):
                prev_rows, next_rows = hrecv[i, 0, u, p], hrecv[i, 1, u, p]
                side.append(jnp.where(low, prev_rows, pltpu.roll(next_rows, 4, 0)))
                side.append(jnp.where(low, pltpu.roll(prev_rows, 4, 0), next_rows))

            def energy(e, sums):
                a = [att[m, e] for m in range(MATS)]
                bright = []
                for part in (own, side):
                    level = (a[0] * part[0] + a[1] * part[1]) + (a[2] * part[2] + a[3] * part[3])
                    bright.append(jnp.exp(-level))
                new = []
                for b in range(CBINS):
                    w = resp[b, e]
                    new.append((sums[b][0] + w * bright[0], sums[b][1] + w * bright[1]))
                return tuple(new)

            start = tuple((jnp.zeros((8, PB), F32),) * 2 for _ in range(CBINS))
            sums = lax.fori_loop(0, EBINS, energy, start, unroll=8)
            for b in range(CBINS):
                own_b, side_b = sums[b]
                side_b = jnp.where(inside, side_b, 0.0)
                share = leak[b]
                value = (1.0 - 2.0 * share) * own_b + share * (pltpu.roll(own_b, 4, 0) + side_b)
                obuf[b, pl.ds(i * 2 + u, 8, stride=16), :] = value

    stages = (
        (0, project), (LAG_EXPAND, expand), (LAG_RELAY, pass_on), (LAG_OWNER, gather),
        (LAG_CROSS, finish), (LAG_DEPTH, across), (LAG_DETECT, detect),
    )

    def step(t, carry):
        for lag, run in stages:
            i = t - lag

            @pl.when((i >= 0) & (i < PAIRS))
            def _(i=i, run=run):
                run(i)

        return carry

    lax.fori_loop(0, PAIRS + LAG_DETECT, step, 0)

    for j in range(2):
        for b in range(4):
            out[:, j, :, pl.ds(b * PB, PB)] = obuf[:, pl.ds((j * 4 + b) * 16, 16), :]

    def drain(i, carry):
        for u in range(2):
            v = i * 2 + u
            give_copy(v).wait_send()
            for d in range(2):
                far_copy(v, u, d).wait_send()
                for half in range(2):
                    near_copy(v, u, d, half).wait_send()
            for r in (1, 2, 3):
                cross_copy(v, u, r).wait_send()
        for d in range(1, 8):
            z_copy(i, d).wait_send()
        for d in range(2):
            h_copy(i, d).wait_send()
        return carry

    lax.fori_loop(0, PAIRS, drain, 0)


def per_device(volume, system, geometry, attenuation, response, crosstalk):
    dma = pltpu.SemaphoreType.DMA
    vmem = pltpu.VMEM
    smem = pl.BlockSpec(memory_space=pltpu.SMEM)
    far = pl.BlockSpec(memory_space=pl.ANY)
    return pl.pallas_call(
        kernel,
        out_shape=jax.ShapeDtypeStruct((CBINS, 2, VIEWS, PIX), F32),
        in_specs=[far, far, smem, smem, smem, smem],
        out_specs=pl.BlockSpec(memory_space=pltpu.VMEM),
        scratch_shapes=[
            vmem((SLICES, VOX), BF16),
            vmem((SLICES, VOX), BF16),
            vmem((VOX, KT, PB), BF16),
            vmem((VIEWS, VOX, 2 * PB), BF16),
            vmem((VIEWS, HALF, 2 * PB), F32),
            vmem((VIEWS, HALF, 2 * PB), F32),
            vmem((VIEWS, HALF, 2 * PB), F32),
            vmem((VIEWS, 4, 4, 16, PIX), F32),
            vmem((VIEWS, 2, 2, 16, PIX), F32),
            vmem((VIEWS, 2, 4, 16, PIX), F32),
            vmem((VIEWS, 4, 16, PIX), F32),
            vmem((VIEWS, 3, 16, PIX), F32),
            vmem((2, 4, 16, PB), F32),
            vmem((PAIRS, 128, PB), F32),
            vmem((PAIRS, 8, 16, PB), F32),
            vmem((PAIRS, MATS, 16, PB), F32),
            vmem((PAIRS, 2, 2, 2, 8, PB), F32),
            vmem((PAIRS, 2, 2, 2, 8, PB), F32),
            vmem((CBINS, 128, PB), F32),
            dma((LOADS + 1,)),
            dma((VIEWS,)),
            dma((VIEWS,)),
            dma((VIEWS, 2)),
            dma((VIEWS, 2)),
            dma((VIEWS, 2, 2)),
            dma((VIEWS, 2, 2)),
            dma((VIEWS, 3)),
            dma((VIEWS, 3)),
            dma((PAIRS, 7)),
            dma((PAIRS, 7)),
            dma((PAIRS, 2)),
            dma((PAIRS, 2)),
        ],
        compiler_params=pltpu.CompilerParams(
            collective_id=0, has_side_effects=True, vmem_limit_bytes=67043328
        ),
    )(
        volume.reshape(SLICES, VOX),
        system.reshape(VOX, KT, PB),
        geometry,
        attenuation,
        response,
        crosstalk,
    )


def solution(mesh):
    in_specs = (P("mat", None, "tile", None), P("tile", None, None, None), P(), P(), P(), P())
    out_specs = P(None, ("mat", "tile"), None, None)
    return jax.shard_map(
        per_device, mesh=mesh, in_specs=in_specs, out_specs=out_specs, check_vma=False
    )
```

```python
import functools

import jax
import jax.numpy as jnp
from jax import lax
from jax.experimental import pallas as pl
from jax.experimental.pallas import tpu as pltpu
from jax.sharding import PartitionSpec as P

MESH = pl.DeviceIdType.MESH
F32 = jnp.float32
BF16 = jnp.bfloat16
I32 = jnp.int32
TOP = 32767
LOG2E = 1.4426950408889634
MIX_ATT = (0, 1, 2, 0, 1, 0)
MIX_PROJ = (0, 0, 0, 1, 1, 2)
MATS = 4
VOX = 1024
VIEWS = 16
KT = 32
PB = 128
PIX = 512
EBINS = 64
CBINS = 8
SLICES = 512
HALF = SLICES // 2
PAIRS = VIEWS // 2
KG = 8
GROUPS = KT // KG
LAG_EXPAND = 1
LAG_RELAY = 2
LAG_OWNER = 3
LAG_CROSS = 4
LAG_DETECT = 6
LAG_COMBINE = 8
OPITCH = 24


def kernel(
    vol_hbm, sys_hbm, geom, att, resp, leak,
    out,
    vol, rows, stage, weights,
    give, keep, take,
    ext, far_out, far_in, near_out, near_in, size_out, size_in,
    owned, cross_out, cross_in, csize_out, csize_in,
    zsort, zsend, zrecv, proj, att_mix, resp_mix, shine, hrecv, obuf,
    load_sem, core_s, core_r, far_s, far_r, near_s, near_r, size_s, size0_r, size1_r,
    cross_s, cross_r, csize_s, csize_r, z_s, z_r, h_s, h_r,
):
    mat = lax.axis_index("mat")
    tile = lax.axis_index("tile")
    core = tile % 2
    x = (tile // 2) % 4
    zh = (tile // 8) % 2
    y = tile // 16
    z = zh * 4 + mat

    def tile_of(yy, zz, xx, cc):
        return ((yy * 2 + zz) * 4 + xx) * 2 + cc

    def x_peer(r):
        return (mat, tile_of(y, zh, (x + r) % 4, core))

    def y_peer(r):
        return (mat, tile_of((y + r) % 4, zh, x, core))

    def z_peer(r):
        zt = (z + r) % 8
        return (zt % 4, tile_of(y, zt // 4, x, core))

    partner = (mat, tile_of(y, zh, x, 1 - core))
    flat = mat * 64 + tile
    after = (flat + 1) % 256
    before = (flat + 255) % 256
    after = (after // 64, after % 64)
    before = (before // 64, before % 64)

    vol_load = pltpu.make_async_copy(vol_hbm, vol, load_sem.at[GROUPS])
    vol_load.start()
    loads = [
        pltpu.make_async_copy(sys_hbm.at[:, pl.ds(g * KG, KG)], stage.at[g], load_sem.at[g])
        for g in range(GROUPS)
    ]
    for load in loads:
        load.start()

    def parts_of(value):
        first = value.astype(BF16)
        rest = value - first.astype(F32)
        second = rest.astype(BF16)
        return first, second, (rest - second.astype(F32)).astype(BF16)

    def iota(shape, axis):
        return lax.broadcasted_iota(I32, shape, axis)

    def mixers():
        wide = len(MIX_ATT) * 32
        column = iota((MATS, wide), 1)
        pick = ((column >> 3) & 3) == iota((MATS, wide), 0)
        level = None
        for p, part in enumerate(parts_of(att[...] * (-LOG2E))):
            chosen = None
            for n, q in enumerate(MIX_ATT):
                if q == p:
                    here = (column >> 5) == n
                    chosen = here if chosen is None else chosen | here
            select = jnp.where(pick & chosen, 1.0, 0.0).astype(BF16)
            term = lax.dot_general(
                part, select, (((0,), (0,)), ((), ())), preferred_element_type=F32
            )
            level = term if level is None else level + term
        ray = iota((EBINS, wide), 1) & 7
        for n in range(8):
            att_mix[pl.ds(n * EBINS, EBINS), :] = jnp.where(ray == n, level, 0.0).astype(BF16)
        spread = jnp.where((iota((EBINS, 256), 1) & 63) == iota((EBINS, 256), 0), 1.0, 0.0)
        block = iota((CBINS, 256), 1) >> 6
        for p, part in enumerate(parts_of(resp[...])[:2]):
            flat_part = jnp.dot(part, spread.astype(BF16), preferred_element_type=F32)
            tall = [jnp.where(block == n, flat_part, 0.0) for n in range(4)]
            resp_mix[pl.ds(p * 32, 32), :] = jnp.concatenate(tall, axis=0).astype(BF16)

    barrier = pltpu.get_barrier_semaphore()
    peers = [partner, after, before]
    peers += [x_peer(r) for r in (1, 2, 3)] + [y_peer(r) for r in (1, 2, 3)]
    peers += [z_peer(r) for r in range(1, 8)]
    for peer in peers:
        pl.semaphore_signal(barrier, inc=1, device_id=peer, device_id_type=MESH)

    r_id = lax.broadcasted_iota(jnp.int32, (SLICES, SLICES), 0)
    s_id = lax.broadcasted_iota(jnp.int32, (SLICES, SLICES), 1)
    r_core = (r_id >> 8) * (2 * core - 1) + (1 - core)
    r_y = ((r_id >> 6) + y) & 3
    r_x = ((r_id >> 4) + x) & 3
    r_mat = (r_id >> 2) & 3
    r_zh = (r_id >> 1) & 1
    want = r_mat * 128 + r_y * 32 + r_zh * 16 + r_x * 4 + r_core * 2 + (r_id & 1)
    order = jnp.where(s_id == want, 1.0, 0.0).astype(BF16)
    mixers()
    vol_load.wait()
    loads[0].wait()
    rows[...] = jnp.dot(order, vol[...], preferred_element_type=F32).astype(BF16)

    def turn_block(g, n):
        near = pl.ds(n * 128, 128)
        turned = jnp.swapaxes(stage[g, near], 0, 1)
        for k in range(KG):
            weights[g * (KG // 2) + k // 2, near, pl.ds((k % 2) * PB, PB)] = turned[k]

    for n in range(VOX // 128):
        turn_block(0, n)
    pl.semaphore_wait(barrier, len(peers))

    def turn(g):
        pltpu.make_async_copy(
            sys_hbm.at[:, pl.ds(pl.multiple_of(g * KG, KG), KG)], stage.at[g], load_sem.at[g]
        ).wait()
        for n in range(VOX // 128):
            turn_block(g, n)

    def send(src, dst, s, r, peer):
        copy = pltpu.make_async_remote_copy(
            src_ref=src, dst_ref=dst, send_sem=s, recv_sem=r, device_id=peer, device_id_type=MESH
        )
        return copy

    def give_copy(v):
        return send(give.at[v], take.at[v], core_s, core_r.at[v // 2], partner)

    def await_all(ref, sem):
        pltpu.make_async_copy(ref, ref, sem).wait()

    def chunk(v, u, r, half):
        if u == 0:
            return ext.at[v, pl.ds(half * 2, 2), r]
        return ext.at[v, r, pl.ds(half * 2, 2)]

    first_peer = (x_peer, y_peer)
    second_peer = (y_peer, x_peer)

    def far_copy(v, u, d):
        return send(far_out.at[v, d], far_in.at[v, d], far_s, far_r.at[v // 2], first_peer[u]((1, 3)[d]))

    def near_copy(v, u, d, late):
        return send(
            near_out.at[v, d, late], near_in.at[v, d, late], near_s, near_r.at[v // 2], first_peer[u]((1, 3)[d])
        )

    def size_copy(v, u, d, late):
        return send(
            size_out.at[late, v, d], size_in.at[late, v, d],
            size_s, (size0_r, size1_r)[late].at[v // 2], first_peer[u]((1, 3)[d]),
        )

    def cross_copy(v, u, r):
        return send(
            cross_out.at[v, r - 1], cross_in.at[v, r - 1], cross_s, cross_r.at[v // 2], second_peer[u](r)
        )

    def csize_copy(v, u, r):
        return send(
            csize_out.at[v, r - 1], csize_in.at[v, r - 1], csize_s, csize_r.at[v // 2], second_peer[u](r)
        )

    def peak(parts):
        top = None
        for part in parts:
            part = jnp.abs(part)
            top = part if top is None else jnp.maximum(top, part)
        return jnp.max(top, axis=0, keepdims=True)

    def code(first, second, inverse):
        first = jnp.round(first * inverse).astype(I32)
        second = jnp.round(second * inverse).astype(I32)
        return (first << 16) + second

    def inverse_of(top):
        return TOP / jnp.maximum(top, 1e-30)

    def decode(word, unit):
        first = (word + 32768) >> 16
        second = word - (first << 16)
        return first.astype(F32) * unit, second.astype(F32) * unit

    def lanes(b):
        return pl.ds(b * PB, PB)

    def z_copy(i, d):
        zt = (z + d) % 8
        q = (zt % 4) * 2 + zt // 4
        return send(
            zsend.at[i, pl.ds(pl.multiple_of(q * 16, 16), 16)],
            zrecv.at[i, z],
            z_s,
            z_r.at[i],
            z_peer(d),
        )

    def h_copy(i, d):
        return send(shine.at[i, 1 - d], hrecv.at[i, d], h_s, h_r.at[i], (after, before)[d])

    def both_views(i):
        return pl.ds(i * 2, 2)

    def project(i):
        for u in range(2):
            v = i * 2 + u
            both = jnp.dot(rows[...], weights[v], preferred_element_type=F32)
            give[v] = both[:HALF]
            give_copy(v).start()
            keep[v] = both[HALF:]

    def expand(i):
        await_all(take.at[both_views(i)], core_r.at[i])
        for u in range(2):
            v = i * 2 + u
            mine = geom[v, tile]
            theirs = geom[v, tile + 1 - 2 * core]
            for n in range(HALF // 16):
                near = pl.ds(n * 16, 16)
                own0, own1 = keep[v, near, pl.ds(0, PB)], keep[v, near, pl.ds(PB, PB)]
                oth0, oth1 = take[v, near, pl.ds(0, PB)], take[v, near, pl.ds(PB, PB)]
                zero = jnp.zeros_like(own0)
                for b in range(4):
                    total = None
                    for first, part0, part1 in ((mine, own0, own1), (theirs, oth0, oth1)):
                        if b == 0:
                            term = jnp.where(first == 0, part0, zero)
                        elif b == 3:
                            term = jnp.where(first == 2, part1, zero)
                        else:
                            term = jnp.where(first == b, part0, jnp.where(first == b - 1, part1, zero))
                        total = term if total is None else total + term
                    ext[v, n // 4, n % 4, :, lanes(b)] = total
            for d in range(2):
                far, near = chunk(v, u, 2, d), chunk(v, u, (1, 3)[d], 1 - d)
                top = peak(
                    part[n, :, lanes(b)] for part in (far, near) for n in range(2) for b in range(4)
                )
                size_out[0, v, d] = top * (1.0 / TOP)
                inverse = inverse_of(top)
                for b in range(4):
                    far_out[v, d, :, lanes(b)] = code(far[0, :, lanes(b)], far[1, :, lanes(b)], inverse)
                size_copy(v, u, d, 0).start()
                far_copy(v, u, d).start()
                for b in range(4):
                    near_out[v, d, 0, :, lanes(b)] = code(near[0, :, lanes(b)], near[1, :, lanes(b)], inverse)
                near_copy(v, u, d, 0).start()

    def pass_on(i):
        await_all(size_in.at[0, both_views(i)], size0_r.at[i])
        await_all(far_in.at[both_views(i)], far_r.at[i])
        for u in range(2):
            v = i * 2 + u
            for d in range(2):
                unit = size_in[0, v, d]
                mine = chunk(v, u, (1, 3)[d], d)
                sums = []
                for b in range(4):
                    first, second = decode(far_in[v, d, :, lanes(b)], unit)
                    sums.append((mine[0, :, lanes(b)] + first, mine[1, :, lanes(b)] + second))
                top = peak(part for both in sums for part in both)
                size_out[1, v, d] = top * (1.0 / TOP)
                inverse = inverse_of(top)
                for b in range(4):
                    near_out[v, d, 1, :, lanes(b)] = code(sums[b][0], sums[b][1], inverse)
                size_copy(v, u, d, 1).start()
                near_copy(v, u, d, 1).start()

    def gather(i):
        await_all(size_in.at[1, both_views(i)], size1_r.at[i])
        await_all(near_in.at[both_views(i)], near_r.at[i])
        for u in range(2):
            v = i * 2 + u
            units = [[size_in[late, v, d] for late in range(2)] for d in range(2)]
            total = [[None] * 4 for _ in range(4)]
            for half in range(2):
                for b in range(4):
                    up = decode(near_in[v, 0, 1 - half, :, lanes(b)], units[0][1 - half])
                    down = decode(near_in[v, 1, half, :, lanes(b)], units[1][half])
                    for k in range(2):
                        n = half * 2 + k
                        mine = ext[v, n, 0, :, lanes(b)] if u == 0 else ext[v, 0, n, :, lanes(b)]
                        total[n][b] = mine + (up[k] + down[k])
            for b in range(4):
                owned[v, :, lanes(b)] = total[0][b]
            for r in (2, 1, 3):
                top = peak(total[r][b][8 * k : 8 * k + 8] for b in range(4) for k in range(2))
                csize_out[v, r - 1] = top * (1.0 / TOP)
                inverse = inverse_of(top)
                for b in range(4):
                    cross_out[v, r - 1, :, lanes(b)] = code(total[r][b][:8], total[r][b][8:], inverse)
                csize_copy(v, u, r).start()
                cross_copy(v, u, r).start()

    def finish(i):
        await_all(csize_in.at[both_views(i)], csize_r.at[i])
        await_all(cross_in.at[both_views(i)], cross_r.at[i])
        for u in range(2):
            v = i * 2 + u
            units = [csize_in[v, r] for r in range(3)]
            for b in range(4):
                got = [decode(cross_in[v, r, :, lanes(b)], units[r]) for r in range(3)]
                for k in range(2):
                    part = owned[v, pl.ds(8 * k, 8), lanes(b)] + (got[0][k] + (got[1][k] + got[2][k]))
                    zsort[u, pl.ds(32 * k + b, 8, stride=4), :] = part
            for q in range(8):
                zsend[i, pl.ds(q * 16 + u * 8, 8), :] = zsort[u, pl.ds(q * 8, 8), :]
        for d in (4, 3, 5, 2, 6, 1, 7):
            z_copy(i, d).start()
        q = mat * 2 + zh
        zrecv[i, z] = zsend[i, pl.ds(pl.multiple_of(q * 16, 16), 16), :]

    def detect(i):
        await_all(zrecv.at[i, pl.ds(0, 7)], z_r.at[i])
        for m in range(MATS):
            both = zrecv[i, m] + zrecv[i, 4 + m]
            for u in range(2):
                proj[pl.ds(m * 8, 8), pl.ds(u * PB, PB)] = both[u * 8 : u * 8 + 8]
        parts = parts_of(proj[...])
        mixed = jnp.concatenate([parts[p] for p in MIX_PROJ], axis=0)
        for j in range(2):
            level = jnp.dot(att_mix[pl.ds(j * 256, 256), :], mixed, preferred_element_type=F32)
            bright = jnp.exp2(level)
            first = bright.astype(BF16)
            second = (bright - first.astype(F32)).astype(BF16)
            large = jnp.dot(resp_mix[...], first, preferred_element_type=F32)
            small = jnp.dot(resp_mix[pl.ds(0, 32), :], second, preferred_element_type=F32)
            shine[i, j] = large[:32] + (large[32:] + small)
        h_copy(i, 0).start()
        h_copy(i, 1).start()

    share = jnp.zeros((CBINS, PB), F32)
    for n in range(CBINS):
        share = jnp.where(iota((CBINS, PB), 0) == n, leak[n], share)
    rest = 1.0 - 2.0 * share
    outer = (flat > 0, flat < 255)

    def combine(i):
        await_all(hrecv.at[i], h_r.at[i])
        for b in range(4):
            near = pl.ds(b * 8, 8)
            own = [shine[i, j, near, :] for j in range(2)]
            for j in range(2):
                side = jnp.where(outer[j], hrecv[i, j, near, :], 0.0)
                for u in range(2):
                    half = slice(u * PB, u * PB + PB)
                    value = rest * own[j][:, half] + share * (own[1 - j][:, half] + side[:, half])
                    obuf[j * 4 + b, pl.ds(i * 2 + u, 8, stride=OPITCH), :] = value

    stages = (
        (0, project), (LAG_EXPAND, expand), (LAG_RELAY, pass_on), (LAG_OWNER, gather),
        (LAG_CROSS, finish), (LAG_DETECT, detect), (LAG_COMBINE, combine),
    )

    def step(t, carry):
        for lag, run in stages:
            i = t - lag

            @pl.when((i >= 0) & (i < PAIRS))
            def _(i=i, run=run):
                run(i)

            if run is project:
                g = (t // 2) + 1

                @pl.when((t % 2 == 0) & (g < GROUPS))
                def _(g=g):
                    turn(g)

        return carry

    lax.fori_loop(0, PAIRS + LAG_COMBINE, step, 0)

    for j in range(2):
        for b in range(4):
            for n in range(CBINS):
                out[n, j, :, lanes(b)] = obuf[j * 4 + b, pl.ds(n * OPITCH, VIEWS), :]

    for ref, sem in (
        (give, core_s), (far_out, far_s), (near_out, near_s), (size_out, size_s), (cross_out, cross_s),
        (csize_out, csize_s), (zsend.at[:, pl.ds(0, 112)], z_s), (shine, h_s),
    ):
        await_all(ref, sem)


def per_device(volume, system, geometry, attenuation, response, crosstalk):
    dma = pltpu.SemaphoreType.DMA
    vmem = pltpu.VMEM
    smem = pl.BlockSpec(memory_space=pltpu.SMEM)
    far = pl.BlockSpec(memory_space=pl.ANY)
    near = pl.BlockSpec(memory_space=pltpu.VMEM)
    return pl.pallas_call(
        kernel,
        out_shape=jax.ShapeDtypeStruct((CBINS, 2, VIEWS, PIX), F32),
        in_specs=[far, far, smem, near, near, smem],
        out_specs=pl.BlockSpec(memory_space=pltpu.VMEM),
        scratch_shapes=[
            vmem((SLICES, VOX), BF16),
            vmem((SLICES, VOX), BF16),
            vmem((GROUPS, VOX, KG, PB), BF16),
            vmem((VIEWS, VOX, 2 * PB), BF16),
            vmem((VIEWS, HALF, 2 * PB), F32),
            vmem((VIEWS, HALF, 2 * PB), F32),
            vmem((VIEWS, HALF, 2 * PB), F32),
            vmem((VIEWS, 4, 4, 16, PIX), F32),
            vmem((VIEWS, 2, 16, PIX), I32),
            vmem((VIEWS, 2, 16, PIX), I32),
            vmem((VIEWS, 2, 2, 16, PIX), I32),
            vmem((VIEWS, 2, 2, 16, PIX), I32),
            vmem((2, VIEWS, 2, 1, PB), F32),
            vmem((2, VIEWS, 2, 1, PB), F32),
            vmem((VIEWS, 16, PIX), F32),
            vmem((VIEWS, 3, 8, PIX), I32),
            vmem((VIEWS, 3, 8, PIX), I32),
            vmem((VIEWS, 3, 1, PB), F32),
            vmem((VIEWS, 3, 1, PB), F32),
            vmem((2, 64, PB), F32),
            vmem((PAIRS, 128, PB), F32),
            vmem((PAIRS, 8, 16, PB), F32),
            vmem((32, 2 * PB), F32),
            vmem((8 * EBINS, len(MIX_ATT) * 32), BF16),
            vmem((64, 256), BF16),
            vmem((PAIRS, 2, 32, 2 * PB), F32),
            vmem((PAIRS, 2, 32, 2 * PB), F32),
            vmem((8, CBINS * OPITCH, PB), F32),
            dma((GROUPS + 1,)),
            dma, dma((PAIRS,)),
            dma, dma((PAIRS,)),
            dma, dma((PAIRS,)),
            dma, dma((PAIRS,)), dma((PAIRS,)),
            dma, dma((PAIRS,)),
            dma, dma((PAIRS,)),
            dma, dma((PAIRS,)),
            dma, dma((PAIRS,)),
        ],
        compiler_params=pltpu.CompilerParams(
            collective_id=0, has_side_effects=True, vmem_limit_bytes=67043328
        ),
    )(
        volume.reshape(SLICES, VOX),
        system.reshape(VOX, KT, PB),
        geometry.T,
        attenuation,
        response,
        crosstalk,
    )


def solution(mesh):
    in_specs = (P("mat", None, "tile", None), P("tile", None, None, None), P(), P(), P(), P())
    out_specs = P(None, ("mat", "tile"), None, None)
    return jax.shard_map(
        per_device, mesh=mesh, in_specs=in_specs, out_specs=out_specs, check_vma=False
    )
```

```python
import functools

import jax
import jax.numpy as jnp
from jax import lax
from jax.experimental import pallas as pl
from jax.experimental.pallas import tpu as pltpu
from jax.sharding import PartitionSpec as P

MESH = pl.DeviceIdType.MESH
F32 = jnp.float32
BF16 = jnp.bfloat16
I32 = jnp.int32
TOP = 32767
LOG2E = 1.4426950408889634
MIX_ATT = (0, 1, 2, 0, 1, 0)
MIX_PROJ = (0, 0, 0, 1, 1, 2)
MATS = 4
VOX = 1024
VIEWS = 16
KT = 32
PB = 128
PIX = 512
EBINS = 64
CBINS = 8
SLICES = 512
HALF = SLICES // 2
PAIRS = VIEWS // 2
KG = 8
GROUPS = KT // KG
LAG_PROJECT = -2
LAG_EXPAND = -1
LAG_RELAY = 1
LAG_OWNER = 2
LAG_CROSS = 3
LAG_DETECT = 5
LAG_COMBINE = 7
MERGE = 2
OPITCH = 24
DIRECT = 2


def kernel(
    vol_hbm, sys_hbm, geom, att, resp, leak,
    out,
    vol, rows, stage, weights,
    give, keep, take,
    ext, far_out, far_in, near_out, near_in, size_out, size_in,
    owned, cross_out, cross_in, csize_out, csize_in,
    zsort, zsend, zrecv, proj, att_mix, resp_mix, shine, hrecv, obuf, hz_out, hz_in, aside,
    load_sem, core_s, core_r, far_s, far_r, near_s, near_r, size_s, size0_r, size1_r,
    cross_s, cross_r, csize_s, csize_r, z_s, z_r, h_s, h_r, hz_s, hz_r, met,
):
    mat = lax.axis_index("mat")
    tile = lax.axis_index("tile")
    core = tile % 2
    x = (tile // 2) % 4
    zh = (tile // 8) % 2
    y = tile // 16
    z = zh * 4 + mat

    def tile_of(yy, zz, xx, cc):
        return ((yy * 2 + zz) * 4 + xx) * 2 + cc

    def x_peer(r):
        return (mat, tile_of(y, zh, (x + r) % 4, core))

    def y_peer(r):
        return (mat, tile_of((y + r) % 4, zh, x, core))

    def z_peer(r):
        zt = (z + r) % 8
        return (zt % 4, tile_of(y, zt // 4, x, core))

    partner = (mat, tile_of(y, zh, x, 1 - core))
    flat = mat * 64 + tile

    def beside(where, d):
        other = (where + (1, 255)[d]) % 256
        return other // 64, other % 64

    after, before = beside(flat, 0), beside(flat, 1)

    vol_load = pltpu.make_async_copy(vol_hbm, vol, load_sem.at[GROUPS])
    vol_load.start()
    loads = [
        pltpu.make_async_copy(sys_hbm.at[:, pl.ds(g * KG, KG)], stage.at[g], load_sem.at[g])
        for g in range(GROUPS)
    ]
    for load in loads:
        load.start()

    def parts_of(value):
        first = value.astype(BF16)
        rest = value - first.astype(F32)
        second = rest.astype(BF16)
        return first, second, (rest - second.astype(F32)).astype(BF16)

    def iota(shape, axis):
        return lax.broadcasted_iota(I32, shape, axis)

    def mixers():
        wide = len(MIX_ATT) * 32
        column = iota((MATS, wide), 1)
        pick = ((column >> 3) & 3) == iota((MATS, wide), 0)
        level = None
        for p, part in enumerate(parts_of(att[...] * (-LOG2E))):
            chosen = None
            for n, q in enumerate(MIX_ATT):
                if q == p:
                    here = (column >> 5) == n
                    chosen = here if chosen is None else chosen | here
            select = jnp.where(pick & chosen, 1.0, 0.0).astype(BF16)
            term = lax.dot_general(
                part, select, (((0,), (0,)), ((), ())), preferred_element_type=F32
            )
            level = term if level is None else level + term
        ray = iota((EBINS, wide), 1) & 7
        for n in range(8):
            att_mix[pl.ds(n * EBINS, EBINS), :] = jnp.where(ray == n, level, 0.0).astype(BF16)
        spread = jnp.where((iota((EBINS, 256), 1) & 63) == iota((EBINS, 256), 0), 1.0, 0.0)
        block = iota((CBINS, 256), 1) >> 6
        for p, part in enumerate(parts_of(resp[...])[:2]):
            flat_part = jnp.dot(part, spread.astype(BF16), preferred_element_type=F32)
            tall = [jnp.where(block == n, flat_part, 0.0) for n in range(4)]
            resp_mix[pl.ds(p * 32, 32), :] = jnp.concatenate(tall, axis=0).astype(BF16)

    barrier = pltpu.get_barrier_semaphore()
    peers = [partner, after, before]
    peers += [x_peer(r) for r in (1, 2, 3)] + [y_peer(r) for r in (1, 2, 3)]
    peers += [z_peer(r) for r in range(1, 8)]
    for peer in peers:
        pl.semaphore_signal(barrier, inc=1, device_id=peer, device_id_type=MESH)

    r_id, s_id = iota((128, 128), 0), iota((128, 128), 1)
    r_core = (r_id >> 6) * (2 * core - 1) + (1 - core)
    r_x = ((r_id >> 4) + x) & 3
    want = ((r_id >> 2) & 3) * 32 + ((r_id >> 1) & 1) * 16 + r_x * 4 + r_core * 2 + (r_id & 1)
    order = jnp.where(s_id == want, 1.0, 0.0).astype(BF16)
    mixers()
    vol_load.wait()
    loads[0].wait()
    for n in range(4):
        base = ((y + n) % 4) * 32
        some = jnp.concatenate(
            [vol[pl.ds(pl.multiple_of(m * 128 + base, 32), 32), :] for m in range(4)], axis=0
        )
        some = jnp.dot(order, some, preferred_element_type=F32).astype(BF16)
        rows[pl.ds(n * 64, 64), :] = some[:64]
        rows[pl.ds(HALF + n * 64, 64), :] = some[64:]

    def turn_block(g, n):
        near = pl.ds(n * 128, 128)
        turned = jnp.swapaxes(stage[g, near], 0, 1)
        for k in range(KG):
            weights[g * (KG // 2) + k // 2, near, pl.ds((k % 2) * PB, PB)] = turned[k]

    for n in range(VOX // 128):
        turn_block(0, n)

    def multiply(i):
        for u in range(2):
            v = i * 2 + u
            both = jnp.dot(rows[...], weights[v], preferred_element_type=F32)
            give[v] = both[:HALF]
            keep[v] = both[HALF:]

    multiply(0)
    pl.semaphore_wait(barrier, len(peers))

    def turn(g):
        pltpu.make_async_copy(
            sys_hbm.at[:, pl.ds(pl.multiple_of(g * KG, KG), KG)], stage.at[g], load_sem.at[g]
        ).wait()
        for n in range(VOX // 128):
            turn_block(g, n)

    def send(src, dst, s, r, peer):
        copy = pltpu.make_async_remote_copy(
            src_ref=src, dst_ref=dst, send_sem=s, recv_sem=r, device_id=peer, device_id_type=MESH
        )
        return copy

    def give_copy(v):
        return send(give.at[v], take.at[v], core_s, core_r.at[v // 2], partner)

    def await_all(ref, sem):
        pltpu.make_async_copy(ref, ref, sem).wait()

    def chunk(v, u, r, half):
        if u == 0:
            return ext.at[v, pl.ds(half * 2, 2), r]
        return ext.at[v, r, pl.ds(half * 2, 2)]

    first_peer = (x_peer, y_peer)
    second_peer = (y_peer, x_peer)

    def far_copy(v, u, d):
        return send(far_out.at[v, d], far_in.at[v, d], far_s, far_r.at[v // 2], first_peer[u]((1, 3)[d]))

    def near_copy(v, u, d, late):
        return send(
            near_out.at[v, d, late], near_in.at[v, d, late], near_s, near_r.at[v // 2], first_peer[u]((1, 3)[d])
        )

    def size_copy(v, u, d, late):
        return send(
            size_out.at[late, v, d], size_in.at[late, v, d],
            size_s, (size0_r, size1_r)[late].at[v // 2], first_peer[u]((1, 3)[d]),
        )

    def cross_copy(v, u, r):
        return send(
            cross_out.at[v, r - 1], cross_in.at[v, r - 1], cross_s, cross_r.at[v // 2], second_peer[u](r)
        )

    def csize_copy(v, u, r):
        return send(
            csize_out.at[v, r - 1], csize_in.at[v, r - 1], csize_s, csize_r.at[v // 2], second_peer[u](r)
        )

    def peak(parts):
        top = None
        for part in parts:
            part = jnp.abs(part)
            top = part if top is None else jnp.maximum(top, part)
        return jnp.max(top, axis=0, keepdims=True)

    def code(first, second, inverse):
        first = jnp.round(first * inverse).astype(I32)
        second = jnp.round(second * inverse).astype(I32)
        return (first << 16) + second

    def inverse_of(top):
        return TOP / jnp.maximum(top, 1e-30)

    def decode(word, unit):
        first = (word + 32768) >> 16
        second = word - (first << 16)
        return first.astype(F32) * unit, second.astype(F32) * unit

    def lanes(b):
        return pl.ds(b * PB, PB)

    def z_copy(i, d):
        zt = (z + d) % 8
        q = (zt % 4) * 2 + zt // 4
        return send(
            zsend.at[i, pl.ds(pl.multiple_of(q * 16, 16), 16)],
            zrecv.at[i, z],
            z_s,
            z_r.at[i],
            z_peer(d),
        )

    def h_copy(i, d):
        return send(shine.at[i, 1 - d], hrecv.at[i, d], h_s, h_r.at[i], (after, before)[d])

    def hz_copy(n, q, d):
        owner = (q // 2) * 64 + tile_of(y, q % 2, x, core)
        return send(
            hz_out.at[n, pl.ds(q * 16 + (1 - d) * 8, 8)], hz_in.at[n, d, z], hz_s, hz_r.at[n], beside(owner, d)
        )

    def both_views(i):
        return pl.ds(i * 2, 2)

    def project(i):
        multiply(i)
        for u in range(2):
            give_copy(i * 2 + u).start()

    def expand(i):
        await_all(take.at[both_views(i)], core_r.at[i])
        for u in range(2):
            v = i * 2 + u
            mine = geom[v, tile]
            theirs = geom[v, tile + 1 - 2 * core]
            for n in range(HALF // 16):
                near = pl.ds(n * 16, 16)
                own0, own1 = keep[v, near, pl.ds(0, PB)], keep[v, near, pl.ds(PB, PB)]
                oth0, oth1 = take[v, near, pl.ds(0, PB)], take[v, near, pl.ds(PB, PB)]
                zero = jnp.zeros_like(own0)
                for b in range(4):
                    total = None
                    for first, part0, part1 in ((mine, own0, own1), (theirs, oth0, oth1)):
                        if b == 0:
                            term = jnp.where(first == 0, part0, zero)
                        elif b == 3:
                            term = jnp.where(first == 2, part1, zero)
                        else:
                            term = jnp.where(first == b, part0, jnp.where(first == b - 1, part1, zero))
                        total = term if total is None else total + term
                    ext[v, n // 4, n % 4, :, lanes(b)] = total
            for d in range(2):
                far, near = chunk(v, u, 2, d), chunk(v, u, (1, 3)[d], 1 - d)
                top = peak(
                    part[n, :, lanes(b)] for part in (far, near) for n in range(2) for b in range(4)
                )
                size_out[0, v, d] = top * (1.0 / TOP)
                inverse = inverse_of(top)
                for b in range(4):
                    far_out[v, d, :, lanes(b)] = code(far[0, :, lanes(b)], far[1, :, lanes(b)], inverse)
                size_copy(v, u, d, 0).start()
                far_copy(v, u, d).start()
                for b in range(4):
                    near_out[v, d, 0, :, lanes(b)] = code(near[0, :, lanes(b)], near[1, :, lanes(b)], inverse)
                near_copy(v, u, d, 0).start()

    def pass_on(i):
        await_all(size_in.at[0, both_views(i)], size0_r.at[i])
        await_all(far_in.at[both_views(i)], far_r.at[i])
        for u in range(2):
            v = i * 2 + u
            for d in range(2):
                unit = size_in[0, v, d]
                mine = chunk(v, u, (1, 3)[d], d)
                sums = []
                for b in range(4):
                    first, second = decode(far_in[v, d, :, lanes(b)], unit)
                    sums.append((mine[0, :, lanes(b)] + first, mine[1, :, lanes(b)] + second))
                top = peak(part for both in sums for part in both)
                size_out[1, v, d] = top * (1.0 / TOP)
                inverse = inverse_of(top)
                for b in range(4):
                    near_out[v, d, 1, :, lanes(b)] = code(sums[b][0], sums[b][1], inverse)
                size_copy(v, u, d, 1).start()
                near_copy(v, u, d, 1).start()

    def gather(i):
        await_all(size_in.at[1, both_views(i)], size1_r.at[i])
        await_all(near_in.at[both_views(i)], near_r.at[i])
        for u in range(2):
            v = i * 2 + u
            units = [[size_in[late, v, d] for late in range(2)] for d in range(2)]
            total = [[None] * 4 for _ in range(4)]
            for half in range(2):
                for b in range(4):
                    up = decode(near_in[v, 0, 1 - half, :, lanes(b)], units[0][1 - half])
                    down = decode(near_in[v, 1, half, :, lanes(b)], units[1][half])
                    for k in range(2):
                        n = half * 2 + k
                        mine = ext[v, n, 0, :, lanes(b)] if u == 0 else ext[v, 0, n, :, lanes(b)]
                        total[n][b] = mine + (up[k] + down[k])
            for b in range(4):
                owned[v, :, lanes(b)] = total[0][b]
            for r in (2, 1, 3):
                top = peak(total[r][b][8 * k : 8 * k + 8] for b in range(4) for k in range(2))
                csize_out[v, r - 1] = top * (1.0 / TOP)
                inverse = inverse_of(top)
                for b in range(4):
                    cross_out[v, r - 1, :, lanes(b)] = code(total[r][b][:8], total[r][b][8:], inverse)
                csize_copy(v, u, r).start()
                cross_copy(v, u, r).start()

    def finish(i):
        await_all(csize_in.at[both_views(i)], csize_r.at[i])
        await_all(cross_in.at[both_views(i)], cross_r.at[i])
        for u in range(2):
            v = i * 2 + u
            units = [csize_in[v, r] for r in range(3)]
            for b in range(4):
                got = [decode(cross_in[v, r, :, lanes(b)], units[r]) for r in range(3)]
                for k in range(2):
                    part = owned[v, pl.ds(8 * k, 8), lanes(b)] + (got[0][k] + (got[1][k] + got[2][k]))
                    zsort[u, pl.ds(32 * k + b, 8, stride=4), :] = part
            for q in range(8):
                zsend[i, pl.ds(q * 16 + u * 8, 8), :] = zsort[u, pl.ds(q * 8, 8), :]

        @pl.when(i >= PAIRS - DIRECT)
        def _():
            n = i - (PAIRS - DIRECT)
            for q in range(8):
                for j in range(2):
                    for u in range(2):
                        hz_out[n, pl.ds(q * 16 + j * 8 + u * 4, 4), :] = zsort[u, pl.ds(q * 8 + j * 4, 4), :]
            for d in range(2):
                for q in range(8):
                    hz_copy(n, q, d).start()

        for d in (4, 3, 5, 2, 6, 1, 7):
            z_copy(i, d).start()
        q = mat * 2 + zh
        zrecv[i, z] = zsend[i, pl.ds(pl.multiple_of(q * 16, 16), 16), :]

    def expose(keep_at):
        parts = parts_of(proj[...])
        mixed = jnp.concatenate([parts[p] for p in MIX_PROJ], axis=0)
        for j in range(2):
            level = jnp.dot(att_mix[pl.ds(j * 256, 256), :], mixed, preferred_element_type=F32)
            bright = jnp.exp2(level)
            first = bright.astype(BF16)
            second = (bright - first.astype(F32)).astype(BF16)
            large = jnp.dot(resp_mix[...], first, preferred_element_type=F32)
            small = jnp.dot(resp_mix[pl.ds(0, 32), :], second, preferred_element_type=F32)
            keep_at(j)[...] = large[:32] + (large[32:] + small)

    def detect(i):
        await_all(zrecv.at[i, pl.ds(0, 7)], z_r.at[i])
        for m in range(MATS):
            both = zrecv[i, m] + zrecv[i, 4 + m]
            for u in range(2):
                proj[pl.ds(m * 8, 8), pl.ds(u * PB, PB)] = both[u * 8 : u * 8 + 8]
        expose(lambda j: shine.at[i, j])

        @pl.when(i < PAIRS - DIRECT)
        def _():
            h_copy(i, 0).start()
            h_copy(i, 1).start()

        @pl.when(i >= PAIRS - DIRECT)
        def _():
            n = i - (PAIRS - DIRECT)
            await_all(hz_in.at[n], hz_r.at[n])
            for m in range(MATS):
                for d in range(2):
                    proj[pl.ds(m * 8, 8), pl.ds(d * PB, PB)] = hz_in[n, d, m] + hz_in[n, d, 4 + m]
            expose(lambda j: aside.at[j])
            for u in range(2):
                merge(i, u, lambda j, near, u=u: aside[u, near, pl.ds(j * PB, PB)])

    share = jnp.zeros((CBINS, PB), F32)
    for n in range(CBINS):
        share = jnp.where(iota((CBINS, PB), 0) == n, leak[n], share)
    rest = 1.0 - 2.0 * share
    outer = (flat > 0, flat < 255)

    def merge(i, u, side_of):
        half = pl.ds(u * PB, PB)
        for b in range(4):
            near = pl.ds(b * 8, 8)
            own = [shine[i, j, near, half] for j in range(2)]
            for j in range(2):
                side = jnp.where(outer[j], side_of(j, near), 0.0)
                value = rest * own[j] + share * (own[1 - j] + side)
                obuf[j * 4 + b, pl.ds(i * 2 + u, 8, stride=OPITCH), :] = value

    def combine(i):
        await_all(hrecv.at[i], h_r.at[i])
        for u in range(2):
            merge(i, u, lambda j, near, u=u: hrecv[i, j, near, pl.ds(u * PB, PB)])

    for u in range(2):
        give_copy(u).start()
    for r in range(1, 8):
        pl.semaphore_signal(met, inc=1, device_id=z_peer(r), device_id_type=MESH)
    project(1)
    turn(1)
    expand(0)

    stages = (
        (LAG_PROJECT, 2, PAIRS, project), (LAG_EXPAND, 1, PAIRS, expand), (LAG_RELAY, 0, PAIRS, pass_on),
        (LAG_OWNER, 0, PAIRS, gather), (LAG_CROSS, 0, PAIRS, finish), (LAG_DETECT, 0, PAIRS, detect),
        (LAG_COMBINE, 0, PAIRS - DIRECT, combine),
    )

    def step(t, carry):
        for lag, first, last, run in stages:

            def reach(n, lag=lag, first=first, last=last):
                done = n - lag + 1
                return jnp.where(done > last - MERGE, last, jnp.maximum(done, first))

            lax.fori_loop(reach(t - 1), reach(t), lambda i, c, run=run: (run(i), c)[1], 0)
            if run is project:

                @pl.when((t == 1) | (t == 3))
                def _():
                    turn((t + 3) // 2)

            if run is pass_on:

                @pl.when(t == 1)
                def _():
                    pl.semaphore_wait(met, 7)

        return carry

    lax.fori_loop(0, PAIRS + LAG_DETECT, step, 0)

    for j in range(2):
        for b in range(4):
            for n in range(CBINS):
                out[n, j, :, lanes(b)] = obuf[j * 4 + b, pl.ds(n * OPITCH, VIEWS), :]

    for ref, sem in (
        (give, core_s), (far_out, far_s), (near_out, near_s), (size_out, size_s), (cross_out, cross_s),
        (csize_out, csize_s), (zsend.at[:, pl.ds(0, 112)], z_s), (shine.at[pl.ds(0, PAIRS - DIRECT)], h_s), (hz_out, hz_s),
    ):
        await_all(ref, sem)


def per_device(volume, system, geometry, attenuation, response, crosstalk):
    dma = pltpu.SemaphoreType.DMA
    vmem = pltpu.VMEM
    smem = pl.BlockSpec(memory_space=pltpu.SMEM)
    far = pl.BlockSpec(memory_space=pl.ANY)
    near = pl.BlockSpec(memory_space=pltpu.VMEM)
    return pl.pallas_call(
        kernel,
        out_shape=jax.ShapeDtypeStruct((CBINS, 2, VIEWS, PIX), F32),
        in_specs=[far, far, smem, near, near, smem],
        out_specs=pl.BlockSpec(memory_space=pltpu.VMEM),
        scratch_shapes=[
            vmem((SLICES, VOX), BF16),
            vmem((SLICES, VOX), BF16),
            vmem((GROUPS, VOX, KG, PB), BF16),
            vmem((VIEWS, VOX, 2 * PB), BF16),
            vmem((VIEWS, HALF, 2 * PB), F32),
            vmem((VIEWS, HALF, 2 * PB), F32),
            vmem((VIEWS, HALF, 2 * PB), F32),
            vmem((VIEWS, 4, 4, 16, PIX), F32),
            vmem((VIEWS, 2, 16, PIX), I32),
            vmem((VIEWS, 2, 16, PIX), I32),
            vmem((VIEWS, 2, 2, 16, PIX), I32),
            vmem((VIEWS, 2, 2, 16, PIX), I32),
            vmem((2, VIEWS, 2, 1, PB), F32),
            vmem((2, VIEWS, 2, 1, PB), F32),
            vmem((VIEWS, 16, PIX), F32),
            vmem((VIEWS, 3, 8, PIX), I32),
            vmem((VIEWS, 3, 8, PIX), I32),
            vmem((VIEWS, 3, 1, PB), F32),
            vmem((VIEWS, 3, 1, PB), F32),
            vmem((2, 64, PB), F32),
            vmem((PAIRS, 128, PB), F32),
            vmem((PAIRS, 8, 16, PB), F32),
            vmem((32, 2 * PB), F32),
            vmem((8 * EBINS, len(MIX_ATT) * 32), BF16),
            vmem((64, 256), BF16),
            vmem((PAIRS, 2, 32, 2 * PB), F32),
            vmem((PAIRS, 2, 32, 2 * PB), F32),
            vmem((8, CBINS * OPITCH, PB), F32),
            vmem((DIRECT, 128, PB), F32),
            vmem((DIRECT, 2, 8, 8, PB), F32),
            vmem((2, 32, 2 * PB), F32),
            dma((GROUPS + 1,)),
            dma, dma((PAIRS,)),
            dma, dma((PAIRS,)),
            dma, dma((PAIRS,)),
            dma, dma((PAIRS,)), dma((PAIRS,)),
            dma, dma((PAIRS,)),
            dma, dma((PAIRS,)),
            dma, dma((PAIRS,)),
            dma, dma((PAIRS,)),
            dma, dma((DIRECT,)),
            pltpu.SemaphoreType.REGULAR,
        ],
        compiler_params=pltpu.CompilerParams(
            collective_id=0, has_side_effects=True, vmem_limit_bytes=56 * 2**20
        ),
    )(
        volume.reshape(SLICES, VOX),
        system.reshape(VOX, KT, PB),
        geometry.T,
        attenuation,
        response,
        crosstalk,
    )


def solution(mesh):
    in_specs = (P("mat", None, "tile", None), P("tile", None, None, None), P(), P(), P(), P())
    out_specs = P(None, ("mat", "tile"), None, None)
    return jax.shard_map(
        per_device, mesh=mesh, in_specs=in_specs, out_specs=out_specs, check_vma=False
    )
```

```python
import functools

import jax
import jax.numpy as jnp
from jax import lax
from jax.experimental import pallas as pl
from jax.experimental.pallas import tpu as pltpu
from jax.sharding import PartitionSpec as P

MESH = pl.DeviceIdType.MESH
F32 = jnp.float32
BF16 = jnp.bfloat16
I32 = jnp.int32
TOP = 32767
LOG2E = 1.4426950408889634
MIX_ATT = (0, 1, 2, 0, 1, 0)
MIX_PROJ = (0, 0, 0, 1, 1, 2)
MATS = 4
VOX = 1024
VIEWS = 16
KT = 32
PB = 128
PIX = 512
EBINS = 64
CBINS = 8
SLICES = 512
HALF = SLICES // 2
PAIRS = VIEWS // 2
KG = 8
GROUPS = KT // KG
LAG_PROJECT = -2
LAG_EXPAND = -1
LAG_RELAY = 1
LAG_OWNER = 2
LAG_CROSS = 3
LAG_DETECT = 5
MERGE = 2
OPITCH = 24


def kernel(
    vol_hbm, sys_hbm, geom, att, resp, leak,
    out,
    vol, rows, stage, weights,
    give, keep, take,
    ext, far_out, far_in, near_out, near_in, size_out, size_in,
    owned, cross_out, cross_in, csize_out, csize_in,
    zsort, deep_out, deep_in, side_in, dsize_out, dsize_in, ssize_in, proj, att_mix, resp_mix, shine, aside, obuf,
    load_sem, core_s, core_r, far_s, far_r, near_s, near_r, size_s, size0_r, size1_r,
    cross_s, cross_r, csize_s, csize_r, deep_s, deep_r, side_s, side_r, dsize_s, dsize_r, ssize_s, ssize_r, met,
):
    mat = lax.axis_index("mat")
    tile = lax.axis_index("tile")
    core = tile % 2
    x = (tile // 2) % 4
    zh = (tile // 8) % 2
    y = tile // 16
    z = zh * 4 + mat

    def tile_of(yy, zz, xx, cc):
        return ((yy * 2 + zz) * 4 + xx) * 2 + cc

    def x_peer(r):
        return (mat, tile_of(y, zh, (x + r) % 4, core))

    def y_peer(r):
        return (mat, tile_of((y + r) % 4, zh, x, core))

    def z_peer(r):
        zt = (z + r) % 8
        return (zt % 4, tile_of(y, zt // 4, x, core))

    partner = (mat, tile_of(y, zh, x, 1 - core))
    flat = mat * 64 + tile

    def beside(where, d):
        other = (where + (1, 255)[d]) % 256
        return other // 64, other % 64

    after, before = beside(flat, 0), beside(flat, 1)

    vol_load = pltpu.make_async_copy(vol_hbm, vol, load_sem.at[GROUPS])
    vol_load.start()
    loads = [
        pltpu.make_async_copy(sys_hbm.at[:, pl.ds(g * KG, KG)], stage.at[g], load_sem.at[g])
        for g in range(GROUPS)
    ]
    for load in loads:
        load.start()

    def parts_of(value):
        first = value.astype(BF16)
        rest = value - first.astype(F32)
        second = rest.astype(BF16)
        return first, second, (rest - second.astype(F32)).astype(BF16)

    def iota(shape, axis):
        return lax.broadcasted_iota(I32, shape, axis)

    def mixers():
        wide = len(MIX_ATT) * 32
        column = iota((MATS, wide), 1)
        pick = ((column >> 3) & 3) == iota((MATS, wide), 0)
        level = None
        for p, part in enumerate(parts_of(att[...] * (-LOG2E))):
            chosen = None
            for n, q in enumerate(MIX_ATT):
                if q == p:
                    here = (column >> 5) == n
                    chosen = here if chosen is None else chosen | here
            select = jnp.where(pick & chosen, 1.0, 0.0).astype(BF16)
            term = lax.dot_general(
                part, select, (((0,), (0,)), ((), ())), preferred_element_type=F32
            )
            level = term if level is None else level + term
        ray = iota((EBINS, wide), 1) & 7
        for n in range(8):
            att_mix[pl.ds(n * EBINS, EBINS), :] = jnp.where(ray == n, level, 0.0).astype(BF16)
        spread = jnp.where((iota((EBINS, 256), 1) & 63) == iota((EBINS, 256), 0), 1.0, 0.0)
        block = iota((CBINS, 256), 1) >> 6
        for p, part in enumerate(parts_of(resp[...])[:2]):
            flat_part = jnp.dot(part, spread.astype(BF16), preferred_element_type=F32)
            tall = [jnp.where(block == n, flat_part, 0.0) for n in range(4)]
            resp_mix[pl.ds(p * 32, 32), :] = jnp.concatenate(tall, axis=0).astype(BF16)

    barrier = pltpu.get_barrier_semaphore()
    peers = [partner, after, before]
    peers += [x_peer(r) for r in (1, 2, 3)] + [y_peer(r) for r in (1, 2, 3)]
    peers += [z_peer(r) for r in range(1, 8)]
    for peer in peers:
        pl.semaphore_signal(barrier, inc=1, device_id=peer, device_id_type=MESH)

    r_id, s_id = iota((128, 128), 0), iota((128, 128), 1)
    r_core = (r_id >> 6) * (2 * core - 1) + (1 - core)
    r_x = ((r_id >> 4) + x) & 3
    want = ((r_id >> 2) & 3) * 32 + ((r_id >> 1) & 1) * 16 + r_x * 4 + r_core * 2 + (r_id & 1)
    order = jnp.where(s_id == want, 1.0, 0.0).astype(BF16)
    mixers()
    vol_load.wait()
    loads[0].wait()
    for n in range(4):
        base = ((y + n) % 4) * 32
        some = jnp.concatenate(
            [vol[pl.ds(pl.multiple_of(m * 128 + base, 32), 32), :] for m in range(4)], axis=0
        )
        some = jnp.dot(order, some, preferred_element_type=F32).astype(BF16)
        rows[pl.ds(n * 64, 64), :] = some[:64]
        rows[pl.ds(HALF + n * 64, 64), :] = some[64:]

    def turn_block(g, n):
        near = pl.ds(n * 128, 128)
        turned = jnp.swapaxes(stage[g, near], 0, 1)
        for k in range(KG):
            weights[g * (KG // 2) + k // 2, near, pl.ds((k % 2) * PB, PB)] = turned[k]

    for n in range(VOX // 128):
        turn_block(0, n)

    def multiply(i):
        for u in range(2):
            v = i * 2 + u
            both = jnp.dot(rows[...], weights[v], preferred_element_type=F32)
            give[v] = both[:HALF]
            keep[v] = both[HALF:]

    multiply(0)
    pl.semaphore_wait(barrier, len(peers))

    def turn(g):
        pltpu.make_async_copy(
            sys_hbm.at[:, pl.ds(pl.multiple_of(g * KG, KG), KG)], stage.at[g], load_sem.at[g]
        ).wait()
        for n in range(VOX // 128):
            turn_block(g, n)

    def send(src, dst, s, r, peer):
        copy = pltpu.make_async_remote_copy(
            src_ref=src, dst_ref=dst, send_sem=s, recv_sem=r, device_id=peer, device_id_type=MESH
        )
        return copy

    def give_copy(v):
        return send(give.at[v], take.at[v], core_s, core_r.at[v // 2], partner)

    def await_all(ref, sem):
        pltpu.make_async_copy(ref, ref, sem).wait()

    def chunk(v, u, r, half):
        if u == 0:
            return ext.at[v, pl.ds(half * 2, 2), r]
        return ext.at[v, r, pl.ds(half * 2, 2)]

    first_peer = (x_peer, y_peer)
    second_peer = (y_peer, x_peer)

    def far_copy(v, u, d):
        return send(far_out.at[v, d], far_in.at[v, d], far_s, far_r.at[v // 2], first_peer[u]((1, 3)[d]))

    def near_copy(v, u, d, late):
        return send(
            near_out.at[v, d, late], near_in.at[v, d, late], near_s, near_r.at[v // 2], first_peer[u]((1, 3)[d])
        )

    def size_copy(v, u, d, late):
        return send(
            size_out.at[late, v, d], size_in.at[late, v, d],
            size_s, (size0_r, size1_r)[late].at[v // 2], first_peer[u]((1, 3)[d]),
        )

    def cross_copy(v, u, r):
        return send(
            cross_out.at[v, r - 1], cross_in.at[v, r - 1], cross_s, cross_r.at[v // 2], second_peer[u](r)
        )

    def csize_copy(v, u, r):
        return send(
            csize_out.at[v, r - 1], csize_in.at[v, r - 1], csize_s, csize_r.at[v // 2], second_peer[u](r)
        )

    def peak(parts):
        top = None
        for part in parts:
            part = jnp.abs(part)
            top = part if top is None else jnp.maximum(top, part)
        return jnp.max(top, axis=0, keepdims=True)

    def code(first, second, inverse):
        first = jnp.round(first * inverse).astype(I32)
        second = jnp.round(second * inverse).astype(I32)
        return (first << 16) + second

    def inverse_of(top):
        return TOP / jnp.maximum(top, 1e-30)

    def decode(word, unit):
        first = (word + 32768) >> 16
        second = word - (first << 16)
        return first.astype(F32) * unit, second.astype(F32) * unit

    def lanes(b):
        return pl.ds(b * PB, PB)

    def deep_pair(i, d):
        zt = (z + d) % 8
        q = (zt % 4) * 2 + zt // 4
        return (
            send(deep_out.at[i, q], deep_in.at[i, z], deep_s, deep_r.at[i], z_peer(d)),
            send(dsize_out.at[i], dsize_in.at[i, z], dsize_s, dsize_r.at[i], z_peer(d)),
        )

    def side_pair(i, q, d):
        owner = (q // 2) * 64 + tile_of(y, q % 2, x, core)
        peer = beside(owner, d)
        return (
            send(deep_out.at[i, q, 1 - d], side_in.at[i, d, z], side_s, side_r.at[i], peer),
            send(dsize_out.at[i], ssize_in.at[i, d, z], ssize_s, ssize_r.at[i], peer),
        )

    def both_views(i):
        return pl.ds(i * 2, 2)

    def project(i):
        multiply(i)
        for u in range(2):
            give_copy(i * 2 + u).start()

    def expand(i):
        await_all(take.at[both_views(i)], core_r.at[i])
        for u in range(2):
            v = i * 2 + u
            mine = geom[v, tile]
            theirs = geom[v, tile + 1 - 2 * core]
            for n in range(HALF // 16):
                near = pl.ds(n * 16, 16)
                own0, own1 = keep[v, near, pl.ds(0, PB)], keep[v, near, pl.ds(PB, PB)]
                oth0, oth1 = take[v, near, pl.ds(0, PB)], take[v, near, pl.ds(PB, PB)]
                zero = jnp.zeros_like(own0)
                for b in range(4):
                    total = None
                    for first, part0, part1 in ((mine, own0, own1), (theirs, oth0, oth1)):
                        if b == 0:
                            term = jnp.where(first == 0, part0, zero)
                        elif b == 3:
                            term = jnp.where(first == 2, part1, zero)
                        else:
                            term = jnp.where(first == b, part0, jnp.where(first == b - 1, part1, zero))
                        total = term if total is None else total + term
                    ext[v, n // 4, n % 4, :, lanes(b)] = total
            for d in range(2):
                far, near = chunk(v, u, 2, d), chunk(v, u, (1, 3)[d], 1 - d)
                top = peak(
                    part[n, :, lanes(b)] for part in (far, near) for n in range(2) for b in range(4)
                )
                size_out[0, v, d] = top * (1.0 / TOP)
                inverse = inverse_of(top)
                for b in range(4):
                    far_out[v, d, :, lanes(b)] = code(far[0, :, lanes(b)], far[1, :, lanes(b)], inverse)
                size_copy(v, u, d, 0).start()
                far_copy(v, u, d).start()
                for b in range(4):
                    near_out[v, d, 0, :, lanes(b)] = code(near[0, :, lanes(b)], near[1, :, lanes(b)], inverse)
                near_copy(v, u, d, 0).start()

    def pass_on(i):
        await_all(size_in.at[0, both_views(i)], size0_r.at[i])
        await_all(far_in.at[both_views(i)], far_r.at[i])
        for u in range(2):
            v = i * 2 + u
            for d in range(2):
                unit = size_in[0, v, d]
                mine = chunk(v, u, (1, 3)[d], d)
                sums = []
                for b in range(4):
                    first, second = decode(far_in[v, d, :, lanes(b)], unit)
                    sums.append((mine[0, :, lanes(b)] + first, mine[1, :, lanes(b)] + second))
                top = peak(part for both in sums for part in both)
                size_out[1, v, d] = top * (1.0 / TOP)
                inverse = inverse_of(top)
                for b in range(4):
                    near_out[v, d, 1, :, lanes(b)] = code(sums[b][0], sums[b][1], inverse)
                size_copy(v, u, d, 1).start()
                near_copy(v, u, d, 1).start()

    def gather(i):
        await_all(size_in.at[1, both_views(i)], size1_r.at[i])
        await_all(near_in.at[both_views(i)], near_r.at[i])
        for u in range(2):
            v = i * 2 + u
            units = [[size_in[late, v, d] for late in range(2)] for d in range(2)]
            total = [[None] * 4 for _ in range(4)]
            for half in range(2):
                for b in range(4):
                    up = decode(near_in[v, 0, 1 - half, :, lanes(b)], units[0][1 - half])
                    down = decode(near_in[v, 1, half, :, lanes(b)], units[1][half])
                    for k in range(2):
                        n = half * 2 + k
                        mine = ext[v, n, 0, :, lanes(b)] if u == 0 else ext[v, 0, n, :, lanes(b)]
                        total[n][b] = mine + (up[k] + down[k])
            for b in range(4):
                owned[v, :, lanes(b)] = total[0][b]
            for r in (2, 1, 3):
                top = peak(total[r][b][8 * k : 8 * k + 8] for b in range(4) for k in range(2))
                csize_out[v, r - 1] = top * (1.0 / TOP)
                inverse = inverse_of(top)
                for b in range(4):
                    cross_out[v, r - 1, :, lanes(b)] = code(total[r][b][:8], total[r][b][8:], inverse)
                csize_copy(v, u, r).start()
                cross_copy(v, u, r).start()

    def finish(i):
        await_all(csize_in.at[both_views(i)], csize_r.at[i])
        await_all(cross_in.at[both_views(i)], cross_r.at[i])
        for u in range(2):
            v = i * 2 + u
            units = [csize_in[v, r] for r in range(3)]
            for b in range(4):
                got = [decode(cross_in[v, r, :, lanes(b)], units[r]) for r in range(3)]
                for k in range(2):
                    part = owned[v, pl.ds(8 * k, 8), lanes(b)] + (got[0][k] + (got[1][k] + got[2][k]))
                    zsort[u, pl.ds(32 * k + b, 8, stride=4), :] = part
        top = peak(zsort[u, pl.ds(8 * n, 8), :] for u in range(2) for n in range(8))
        dsize_out[i] = top * (1.0 / TOP)
        word = code(zsort[0], zsort[1], inverse_of(top))
        for q in range(8):
            for j in range(2):
                deep_out[i, q, j] = word[q * 8 + j * 4 : q * 8 + j * 4 + 4]
        for d in range(2):
            for q in range(8):
                for copy in side_pair(i, q, d):
                    copy.start()
        for d in (4, 3, 5, 2, 6, 1, 7):
            for copy in deep_pair(i, d):
                copy.start()
        deep_in[i, z] = deep_out[i, mat * 2 + zh]
        dsize_in[i, z] = dsize_out[i]

    def expose(target):
        parts = parts_of(proj[...])
        mixed = jnp.concatenate([parts[p] for p in MIX_PROJ], axis=0)
        for j in range(2):
            level = jnp.dot(att_mix[pl.ds(j * 256, 256), :], mixed, preferred_element_type=F32)
            bright = jnp.exp2(level)
            first = bright.astype(BF16)
            second = (bright - first.astype(F32)).astype(BF16)
            large = jnp.dot(resp_mix[...], first, preferred_element_type=F32)
            small = jnp.dot(resp_mix[pl.ds(0, 32), :], second, preferred_element_type=F32)
            target[j] = large[:32] + (large[32:] + small)

    def detect(i):
        await_all(dsize_in.at[i, pl.ds(0, 7)], dsize_r.at[i])
        await_all(deep_in.at[i, pl.ds(0, 7)], deep_r.at[i])
        for m in range(MATS):
            for j in range(2):
                one = decode(deep_in[i, m, j], dsize_in[i, m])
                two = decode(deep_in[i, 4 + m, j], dsize_in[i, 4 + m])
                for u in range(2):
                    proj[pl.ds(m * 8 + j * 4, 4), lanes(u)] = one[u] + two[u]
        expose(shine)
        await_all(ssize_in.at[i], ssize_r.at[i])
        await_all(side_in.at[i], side_r.at[i])
        for m in range(MATS):
            for d in range(2):
                one = decode(side_in[i, d, m], ssize_in[i, d, m])
                two = decode(side_in[i, d, 4 + m], ssize_in[i, d, 4 + m])
                for u in range(2):
                    proj[pl.ds(m * 8 + d * 4, 4), lanes(u)] = one[u] + two[u]
        expose(aside)
        for b in range(4):
            near = pl.ds(b * 8, 8)
            for u in range(2):
                own = [shine[j, near, lanes(u)] for j in range(2)]
                for j in range(2):
                    side = jnp.where(outer[j], aside[j, near, lanes(u)], 0.0)
                    value = rest * own[j] + share * (own[1 - j] + side)
                    obuf[j * 4 + b, pl.ds(i * 2 + u, 8, stride=OPITCH), :] = value

    share = jnp.zeros((CBINS, PB), F32)
    for n in range(CBINS):
        share = jnp.where(iota((CBINS, PB), 0) == n, leak[n], share)
    rest = 1.0 - 2.0 * share
    outer = (flat > 0, flat < 255)

    for u in range(2):
        give_copy(u).start()
    for r in range(1, 8):
        pl.semaphore_signal(met, inc=1, device_id=z_peer(r), device_id_type=MESH)
    project(1)
    turn(1)
    expand(0)

    stages = (
        (LAG_PROJECT, 2, PAIRS, project), (LAG_EXPAND, 1, PAIRS, expand), (LAG_RELAY, 0, PAIRS, pass_on),
        (LAG_OWNER, 0, PAIRS, gather), (LAG_CROSS, 0, PAIRS, finish), (LAG_DETECT, 0, PAIRS, detect),
    )

    def step(t, carry):
        for lag, first, last, run in stages:

            def reach(n, lag=lag, first=first, last=last):
                done = n - lag + 1
                return jnp.where(done > last - MERGE, last, jnp.maximum(done, first))

            lax.fori_loop(reach(t - 1), reach(t), lambda i, c, run=run: (run(i), c)[1], 0)
            if run is project:

                @pl.when((t == 1) | (t == 3))
                def _():
                    turn((t + 3) // 2)

            if run is pass_on:

                @pl.when(t == 1)
                def _():
                    pl.semaphore_wait(met, 7)

        return carry

    lax.fori_loop(0, PAIRS + LAG_DETECT, step, 0)

    for j in range(2):
        for b in range(4):
            for n in range(CBINS):
                out[n, j, :, lanes(b)] = obuf[j * 4 + b, pl.ds(n * OPITCH, VIEWS), :]

    for ref, sem in (
        (give, core_s), (far_out, far_s), (near_out, near_s), (size_out, size_s), (cross_out, cross_s),
        (csize_out, csize_s), (deep_out.at[:, pl.ds(0, 7)], deep_s), (side_in, side_s),
        (dsize_in.at[:, pl.ds(0, 7)], dsize_s), (ssize_in, ssize_s),
    ):
        await_all(ref, sem)


def per_device(volume, system, geometry, attenuation, response, crosstalk):
    dma = pltpu.SemaphoreType.DMA
    vmem = pltpu.VMEM
    smem = pl.BlockSpec(memory_space=pltpu.SMEM)
    far = pl.BlockSpec(memory_space=pl.ANY)
    near = pl.BlockSpec(memory_space=pltpu.VMEM)
    return pl.pallas_call(
        kernel,
        out_shape=jax.ShapeDtypeStruct((CBINS, 2, VIEWS, PIX), F32),
        in_specs=[far, far, smem, near, near, smem],
        out_specs=pl.BlockSpec(memory_space=pltpu.VMEM),
        scratch_shapes=[
            vmem((SLICES, VOX), BF16),
            vmem((SLICES, VOX), BF16),
            vmem((GROUPS, VOX, KG, PB), BF16),
            vmem((VIEWS, VOX, 2 * PB), BF16),
            vmem((VIEWS, HALF, 2 * PB), F32),
            vmem((VIEWS, HALF, 2 * PB), F32),
            vmem((VIEWS, HALF, 2 * PB), F32),
            vmem((VIEWS, 4, 4, 16, PIX), F32),
            vmem((VIEWS, 2, 16, PIX), I32),
            vmem((VIEWS, 2, 16, PIX), I32),
            vmem((VIEWS, 2, 2, 16, PIX), I32),
            vmem((VIEWS, 2, 2, 16, PIX), I32),
            vmem((2, VIEWS, 2, 1, PB), F32),
            vmem((2, VIEWS, 2, 1, PB), F32),
            vmem((VIEWS, 16, PIX), F32),
            vmem((VIEWS, 3, 8, PIX), I32),
            vmem((VIEWS, 3, 8, PIX), I32),
            vmem((VIEWS, 3, 1, PB), F32),
            vmem((VIEWS, 3, 1, PB), F32),
            vmem((2, 64, PB), F32),
            vmem((PAIRS, 8, 2, 4, PB), I32),
            vmem((PAIRS, 8, 2, 4, PB), I32),
            vmem((PAIRS, 2, 8, 4, PB), I32),
            vmem((PAIRS, 1, PB), F32),
            vmem((PAIRS, 8, 1, PB), F32),
            vmem((PAIRS, 2, 8, 1, PB), F32),
            vmem((32, 2 * PB), F32),
            vmem((8 * EBINS, len(MIX_ATT) * 32), BF16),
            vmem((64, 256), BF16),
            vmem((2, 32, 2 * PB), F32),
            vmem((2, 32, 2 * PB), F32),
            vmem((8, CBINS * OPITCH, PB), F32),
            dma((GROUPS + 1,)),
            dma, dma((PAIRS,)),
            dma, dma((PAIRS,)),
            dma, dma((PAIRS,)),
            dma, dma((PAIRS,)), dma((PAIRS,)),
            dma, dma((PAIRS,)),
            dma, dma((PAIRS,)),
            dma, dma((PAIRS,)),
            dma, dma((PAIRS,)),
            dma, dma((PAIRS,)),
            dma, dma((PAIRS,)),
            pltpu.SemaphoreType.REGULAR,
        ],
        compiler_params=pltpu.CompilerParams(
            collective_id=0, has_side_effects=True, vmem_limit_bytes=56 * 2**20
        ),
    )(
        volume.reshape(SLICES, VOX),
        system.reshape(VOX, KT, PB),
        geometry.T,
        attenuation,
        response,
        crosstalk,
    )


def solution(mesh):
    in_specs = (P("mat", None, "tile", None), P("tile", None, None, None), P(), P(), P(), P())
    out_specs = P(None, ("mat", "tile"), None, None)
    return jax.shard_map(
        per_device, mesh=mesh, in_specs=in_specs, out_specs=out_specs, check_vma=False
    )
```

```python
import functools

import jax
import jax.numpy as jnp
from jax import lax
from jax.experimental import pallas as pl
from jax.experimental.pallas import tpu as pltpu
from jax.sharding import PartitionSpec as P

MESH = pl.DeviceIdType.MESH
F32 = jnp.float32
BF16 = jnp.bfloat16
I32 = jnp.int32
TOP = 32767
LOG2E = 1.4426950408889634
MIX_ATT = (0, 1, 2, 0, 1, 0)
MIX_PROJ = (0, 0, 0, 1, 1, 2)
MATS = 4
VOX = 1024
VIEWS = 16
KT = 32
PB = 128
PIX = 512
EBINS = 64
CBINS = 8
SLICES = 512
HALF = SLICES // 2
PAIRS = VIEWS // 2
KG = 8
GROUPS = KT // KG
LAG_PROJECT = -2
LAG_EXPAND = -1
LAG_RELAY = 1
LAG_OWNER = 3
LAG_CROSS = 4
LAG_DETECT = 6
OPITCH = 24


def kernel(
    vol_hbm, sys_hbm, geom, att, resp, leak,
    out,
    vol, rows, stage, weights,
    give, keep, take,
    ext, far_out, far_in, near_out, near_in, size_out, size_in,
    owned, cross_out, cross_in, csize_out, csize_in,
    zsort, deep_out, deep_in, side_in, dsize_out, dsize_in, ssize_in, proj, att_mix, resp_mix, shine, aside, obuf,
    load_sem, core_s, core_r, far_s, far_r, near_s, near_r, size_s, size0_r, size1_r,
    cross_s, cross_r, csize_s, csize_r, deep_s, deep_r, side_s, side_r, dsize_s, dsize_r, ssize_s, ssize_r, met,
):
    mat = lax.axis_index("mat")
    tile = lax.axis_index("tile")
    core = tile % 2
    x = (tile // 2) % 4
    zh = (tile // 8) % 2
    y = tile // 16
    z = zh * 4 + mat

    def tile_of(yy, zz, xx, cc):
        return ((yy * 2 + zz) * 4 + xx) * 2 + cc

    def x_peer(r):
        return (mat, tile_of(y, zh, (x + r) % 4, core))

    def y_peer(r):
        return (mat, tile_of((y + r) % 4, zh, x, core))

    def z_peer(r):
        zt = (z + r) % 8
        return (zt % 4, tile_of(y, zt // 4, x, core))

    partner = (mat, tile_of(y, zh, x, 1 - core))
    flat = mat * 64 + tile

    def beside(where, d):
        other = (where + (1, 255)[d]) % 256
        return other // 64, other % 64

    after, before = beside(flat, 0), beside(flat, 1)

    vol_load = pltpu.make_async_copy(vol_hbm, vol, load_sem.at[GROUPS])
    vol_load.start()
    loads = [
        pltpu.make_async_copy(sys_hbm.at[:, pl.ds(g * KG, KG)], stage.at[g], load_sem.at[g])
        for g in range(GROUPS)
    ]
    for load in loads:
        load.start()

    def parts_of(value):
        first = value.astype(BF16)
        rest = value - first.astype(F32)
        second = rest.astype(BF16)
        return first, second, (rest - second.astype(F32)).astype(BF16)

    def iota(shape, axis):
        return lax.broadcasted_iota(I32, shape, axis)

    def mixers():
        wide = len(MIX_ATT) * 32
        column = iota((MATS, wide), 1)
        pick = ((column >> 3) & 3) == iota((MATS, wide), 0)
        level = None
        for p, part in enumerate(parts_of(att[...] * (-LOG2E))):
            chosen = None
            for n, q in enumerate(MIX_ATT):
                if q == p:
                    here = (column >> 5) == n
                    chosen = here if chosen is None else chosen | here
            select = jnp.where(pick & chosen, 1.0, 0.0).astype(BF16)
            term = lax.dot_general(
                part, select, (((0,), (0,)), ((), ())), preferred_element_type=F32
            )
            level = term if level is None else level + term
        ray = iota((EBINS, wide), 1) & 7
        for n in range(8):
            att_mix[pl.ds(n * EBINS, EBINS), :] = jnp.where(ray == n, level, 0.0).astype(BF16)
        spread = jnp.where((iota((EBINS, 256), 1) & 63) == iota((EBINS, 256), 0), 1.0, 0.0)
        block = iota((CBINS, 256), 1) >> 6
        for p, part in enumerate(parts_of(resp[...])[:2]):
            flat_part = jnp.dot(part, spread.astype(BF16), preferred_element_type=F32)
            tall = [jnp.where(block == n, flat_part, 0.0) for n in range(4)]
            resp_mix[pl.ds(p * 32, 32), :] = jnp.concatenate(tall, axis=0).astype(BF16)

    barrier = pltpu.get_barrier_semaphore()
    peers = [partner, after, before]
    peers += [x_peer(r) for r in (1, 2, 3)] + [y_peer(r) for r in (1, 2, 3)]
    peers += [z_peer(r) for r in range(1, 8)]
    for peer in peers:
        pl.semaphore_signal(barrier, inc=1, device_id=peer, device_id_type=MESH)

    r_id, s_id = iota((128, 128), 0), iota((128, 128), 1)
    r_core = (r_id >> 6) * (2 * core - 1) + (1 - core)
    r_x = ((r_id >> 4) + x) & 3
    want = ((r_id >> 2) & 3) * 32 + ((r_id >> 1) & 1) * 16 + r_x * 4 + r_core * 2 + (r_id & 1)
    order = jnp.where(s_id == want, 1.0, 0.0).astype(BF16)
    mixers()
    vol_load.wait()
    loads[0].wait()
    for n in range(4):
        base = ((y + n) % 4) * 32
        some = jnp.concatenate(
            [vol[pl.ds(pl.multiple_of(m * 128 + base, 32), 32), :] for m in range(4)], axis=0
        )
        some = jnp.dot(order, some, preferred_element_type=F32).astype(BF16)
        rows[pl.ds(n * 64, 64), :] = some[:64]
        rows[pl.ds(HALF + n * 64, 64), :] = some[64:]

    def turn_block(g, n):
        near = pl.ds(n * 128, 128)
        turned = jnp.swapaxes(stage[g, near], 0, 1)
        for k in range(KG):
            weights[g * (KG // 2) + k // 2, near, pl.ds((k % 2) * PB, PB)] = turned[k]

    for n in range(VOX // 128):
        turn_block(0, n)

    def multiply(i):
        for u in range(2):
            v = i * 2 + u
            both = jnp.dot(rows[...], weights[v], preferred_element_type=F32)
            give[v] = both[:HALF]
            keep[v] = both[HALF:]

    multiply(0)
    pl.semaphore_wait(barrier, len(peers))

    def turn(g):
        pltpu.make_async_copy(
            sys_hbm.at[:, pl.ds(pl.multiple_of(g * KG, KG), KG)], stage.at[g], load_sem.at[g]
        ).wait()
        for n in range(VOX // 128):
            turn_block(g, n)

    def send(src, dst, s, r, peer):
        copy = pltpu.make_async_remote_copy(
            src_ref=src, dst_ref=dst, send_sem=s, recv_sem=r, device_id=peer, device_id_type=MESH
        )
        return copy

    def give_copy(v):
        return send(give.at[v], take.at[v], core_s, core_r.at[v // 2], partner)

    def await_all(ref, sem):
        pltpu.make_async_copy(ref, ref, sem).wait()

    def chunk(v, u, r, half):
        if u == 0:
            return ext.at[v, pl.ds(half * 2, 2), r]
        return ext.at[v, r, pl.ds(half * 2, 2)]

    first_peer = (x_peer, y_peer)
    second_peer = (y_peer, x_peer)

    def far_copy(v, u, d):
        return send(far_out.at[v, d], far_in.at[v, d], far_s, far_r.at[v // 2], first_peer[u]((1, 3)[d]))

    def near_copy(v, u, d, late):
        return send(
            near_out.at[v, d, late], near_in.at[v, d, late], near_s, near_r.at[v // 2], first_peer[u]((1, 3)[d])
        )

    def size_copy(v, u, d, late):
        return send(
            size_out.at[late, v, d], size_in.at[late, v, d],
            size_s, (size0_r, size1_r)[late].at[v // 2], first_peer[u]((1, 3)[d]),
        )

    def cross_copy(v, u, r):
        return send(
            cross_out.at[v, r - 1], cross_in.at[v, r - 1], cross_s, cross_r.at[v // 2], second_peer[u](r)
        )

    def csize_copy(v, u, r):
        return send(
            csize_out.at[v, r - 1], csize_in.at[v, r - 1], csize_s, csize_r.at[v // 2], second_peer[u](r)
        )

    def peak(parts):
        top = None
        for part in parts:
            part = jnp.abs(part)
            top = part if top is None else jnp.maximum(top, part)
        return jnp.max(top, axis=0, keepdims=True)

    def code(first, second, inverse):
        first = jnp.round(first * inverse).astype(I32)
        second = jnp.round(second * inverse).astype(I32)
        return (first << 16) + second

    def inverse_of(top):
        return TOP / jnp.maximum(top, 1e-30)

    def decode(word, unit):
        first = (word + 32768) >> 16
        second = word - (first << 16)
        return first.astype(F32) * unit, second.astype(F32) * unit

    def lanes(b):
        return pl.ds(b * PB, PB)

    def deep_pair(i, d):
        zt = (z + d) % 8
        q = (zt % 4) * 2 + zt // 4
        return (
            send(deep_out.at[i, q], deep_in.at[i, z], deep_s, deep_r.at[i], z_peer(d)),
            send(dsize_out.at[i], dsize_in.at[i, z], dsize_s, dsize_r.at[i], z_peer(d)),
        )

    def side_pair(i, q, d):
        owner = (q // 2) * 64 + tile_of(y, q % 2, x, core)
        peer = beside(owner, d)
        return (
            send(deep_out.at[i, q, 1 - d], side_in.at[i, d, z], side_s, side_r.at[i], peer),
            send(dsize_out.at[i], ssize_in.at[i, d, z], ssize_s, ssize_r.at[i], peer),
        )

    def both_views(i):
        return pl.ds(i * 2, 2)

    def project(i):
        multiply(i)
        for u in range(2):
            give_copy(i * 2 + u).start()

    def expand(i):
        await_all(take.at[both_views(i)], core_r.at[i])
        for u in range(2):
            v = i * 2 + u
            mine = geom[v, tile]
            theirs = geom[v, tile + 1 - 2 * core]
            for n in range(HALF // 16):
                near = pl.ds(n * 16, 16)
                own0, own1 = keep[v, near, pl.ds(0, PB)], keep[v, near, pl.ds(PB, PB)]
                oth0, oth1 = take[v, near, pl.ds(0, PB)], take[v, near, pl.ds(PB, PB)]
                zero = jnp.zeros_like(own0)
                for b in range(4):
                    total = None
                    for first, part0, part1 in ((mine, own0, own1), (theirs, oth0, oth1)):
                        if b == 0:
                            term = jnp.where(first == 0, part0, zero)
                        elif b == 3:
                            term = jnp.where(first == 2, part1, zero)
                        else:
                            term = jnp.where(first == b, part0, jnp.where(first == b - 1, part1, zero))
                        total = term if total is None else total + term
                    ext[v, n // 4, n % 4, :, lanes(b)] = total
            for d in range(2):
                far, near = chunk(v, u, 2, d), chunk(v, u, (1, 3)[d], 1 - d)
                top = peak(
                    part[n, :, lanes(b)] for part in (far, near) for n in range(2) for b in range(4)
                )
                size_out[0, v, d] = top * (1.0 / TOP)
                inverse = inverse_of(top)
                for b in range(4):
                    far_out[v, d, :, lanes(b)] = code(far[0, :, lanes(b)], far[1, :, lanes(b)], inverse)
                size_copy(v, u, d, 0).start()
                far_copy(v, u, d).start()
                for b in range(4):
                    near_out[v, d, 0, :, lanes(b)] = code(near[0, :, lanes(b)], near[1, :, lanes(b)], inverse)
                near_copy(v, u, d, 0).start()

    def pass_on(i):
        await_all(size_in.at[0, both_views(i)], size0_r.at[i])
        await_all(far_in.at[both_views(i)], far_r.at[i])
        for u in range(2):
            v = i * 2 + u
            for d in range(2):
                unit = size_in[0, v, d]
                mine = chunk(v, u, (1, 3)[d], d)
                sums = []
                for b in range(4):
                    first, second = decode(far_in[v, d, :, lanes(b)], unit)
                    sums.append((mine[0, :, lanes(b)] + first, mine[1, :, lanes(b)] + second))
                top = peak(part for both in sums for part in both)
                size_out[1, v, d] = top * (1.0 / TOP)
                inverse = inverse_of(top)
                for b in range(4):
                    near_out[v, d, 1, :, lanes(b)] = code(sums[b][0], sums[b][1], inverse)
                size_copy(v, u, d, 1).start()
                near_copy(v, u, d, 1).start()

    def gather(i):
        await_all(size_in.at[1, both_views(i)], size1_r.at[i])
        await_all(near_in.at[both_views(i)], near_r.at[i])
        for u in range(2):
            v = i * 2 + u
            units = [[size_in[late, v, d] for late in range(2)] for d in range(2)]
            total = [[None] * 4 for _ in range(4)]
            for half in range(2):
                for b in range(4):
                    up = decode(near_in[v, 0, 1 - half, :, lanes(b)], units[0][1 - half])
                    down = decode(near_in[v, 1, half, :, lanes(b)], units[1][half])
                    for k in range(2):
                        n = half * 2 + k
                        mine = ext[v, n, 0, :, lanes(b)] if u == 0 else ext[v, 0, n, :, lanes(b)]
                        total[n][b] = mine + (up[k] + down[k])
            for b in range(4):
                owned[v, :, lanes(b)] = total[0][b]
            for r in (2, 1, 3):
                top = peak(total[r][b][8 * k : 8 * k + 8] for b in range(4) for k in range(2))
                csize_out[v, r - 1] = top * (1.0 / TOP)
                inverse = inverse_of(top)
                for b in range(4):
                    cross_out[v, r - 1, :, lanes(b)] = code(total[r][b][:8], total[r][b][8:], inverse)
                csize_copy(v, u, r).start()
                cross_copy(v, u, r).start()

    def finish(i):
        await_all(csize_in.at[both_views(i)], csize_r.at[i])
        await_all(cross_in.at[both_views(i)], cross_r.at[i])
        for u in range(2):
            v = i * 2 + u
            units = [csize_in[v, r] for r in range(3)]
            for b in range(4):
                got = [decode(cross_in[v, r, :, lanes(b)], units[r]) for r in range(3)]
                for k in range(2):
                    part = owned[v, pl.ds(8 * k, 8), lanes(b)] + (got[0][k] + (got[1][k] + got[2][k]))
                    zsort[u, pl.ds(32 * k + b, 8, stride=4), :] = part
        top = peak(zsort[u, pl.ds(8 * n, 8), :] for u in range(2) for n in range(8))
        dsize_out[i] = top * (1.0 / TOP)
        word = code(zsort[0], zsort[1], inverse_of(top))
        for q in range(8):
            for j in range(2):
                deep_out[i, q, j] = word[q * 8 + j * 4 : q * 8 + j * 4 + 4]
        for d in range(2):
            for q in range(8):
                for copy in side_pair(i, q, d):
                    copy.start()
        for d in (4, 3, 5, 2, 6, 1, 7):
            for copy in deep_pair(i, d):
                copy.start()
        deep_in[i, z] = deep_out[i, mat * 2 + zh]
        dsize_in[i, z] = dsize_out[i]

    def expose(target):
        parts = parts_of(proj[...])
        mixed = jnp.concatenate([parts[p] for p in MIX_PROJ], axis=0)
        for j in range(2):
            level = jnp.dot(att_mix[pl.ds(j * 256, 256), :], mixed, preferred_element_type=F32)
            bright = jnp.exp2(level)
            first = bright.astype(BF16)
            second = (bright - first.astype(F32)).astype(BF16)
            large = jnp.dot(resp_mix[...], first, preferred_element_type=F32)
            small = jnp.dot(resp_mix[pl.ds(0, 32), :], second, preferred_element_type=F32)
            target[j] = large[:32] + (large[32:] + small)

    def detect(i):
        await_all(dsize_in.at[i, pl.ds(0, 7)], dsize_r.at[i])
        await_all(deep_in.at[i, pl.ds(0, 7)], deep_r.at[i])
        for m in range(MATS):
            for j in range(2):
                one = decode(deep_in[i, m, j], dsize_in[i, m])
                two = decode(deep_in[i, 4 + m, j], dsize_in[i, 4 + m])
                for u in range(2):
                    proj[pl.ds(m * 8 + j * 4, 4), lanes(u)] = one[u] + two[u]
        expose(shine)
        await_all(ssize_in.at[i], ssize_r.at[i])
        await_all(side_in.at[i], side_r.at[i])
        for m in range(MATS):
            for d in range(2):
                one = decode(side_in[i, d, m], ssize_in[i, d, m])
                two = decode(side_in[i, d, 4 + m], ssize_in[i, d, 4 + m])
                for u in range(2):
                    proj[pl.ds(m * 8 + d * 4, 4), lanes(u)] = one[u] + two[u]
        expose(aside)
        for b in range(4):
            near = pl.ds(b * 8, 8)
            for u in range(2):
                own = [shine[j, near, lanes(u)] for j in range(2)]
                for j in range(2):
                    side = jnp.where(outer[j], aside[j, near, lanes(u)], 0.0)
                    value = rest * own[j] + share * (own[1 - j] + side)
                    obuf[j * 4 + b, pl.ds(i * 2 + u, 8, stride=OPITCH), :] = value

    share = jnp.zeros((CBINS, PB), F32)
    for n in range(CBINS):
        share = jnp.where(iota((CBINS, PB), 0) == n, leak[n], share)
    rest = 1.0 - 2.0 * share
    outer = (flat > 0, flat < 255)

    for u in range(2):
        give_copy(u).start()
    for r in range(1, 8):
        pl.semaphore_signal(met, inc=1, device_id=z_peer(r), device_id_type=MESH)
    project(1)
    turn(1)
    expand(0)

    stages = (
        (LAG_PROJECT, 2, 2, project), (LAG_EXPAND, 1, 2, expand), (LAG_RELAY, 0, 3, pass_on),
        (LAG_OWNER, 0, 4, gather), (LAG_CROSS, 0, 2, finish), (LAG_DETECT, 0, 3, detect),
    )

    def step(t, carry):
        for lag, first, merge, run in stages:

            def reach(n, lag=lag, first=first, merge=merge):
                done = n - lag + 1
                return jnp.where(done > PAIRS - merge, PAIRS, jnp.maximum(done, first))

            lax.fori_loop(reach(t - 1), reach(t), lambda i, c, run=run: (run(i), c)[1], 0)
            if run is project:

                @pl.when((t == 1) | (t == 3))
                def _():
                    turn((t + 3) // 2)

            if run is pass_on:

                @pl.when(t == 1)
                def _():
                    pl.semaphore_wait(met, 7)

        return carry

    lax.fori_loop(0, PAIRS + LAG_DETECT - 2, step, 0)

    for j in range(2):
        for b in range(4):
            for n in range(CBINS):
                out[n, j, :, lanes(b)] = obuf[j * 4 + b, pl.ds(n * OPITCH, VIEWS), :]

    for ref, sem in (
        (give, core_s), (far_out, far_s), (near_out, near_s), (size_out, size_s), (cross_out, cross_s),
        (csize_out, csize_s), (deep_out.at[:, pl.ds(0, 7)], deep_s), (side_in, side_s),
        (dsize_in.at[:, pl.ds(0, 7)], dsize_s), (ssize_in, ssize_s),
    ):
        await_all(ref, sem)


def per_device(volume, system, geometry, attenuation, response, crosstalk):
    dma = pltpu.SemaphoreType.DMA
    vmem = pltpu.VMEM
    smem = pl.BlockSpec(memory_space=pltpu.SMEM)
    far = pl.BlockSpec(memory_space=pl.ANY)
    near = pl.BlockSpec(memory_space=pltpu.VMEM)
    return pl.pallas_call(
        kernel,
        out_shape=pltpu.VMEM((CBINS, 2, VIEWS, PIX), F32),
        in_specs=[far, far, smem, near, near, smem],
        out_specs=pl.BlockSpec(memory_space=pltpu.VMEM),
        scratch_shapes=[
            vmem((SLICES, VOX), BF16),
            vmem((SLICES, VOX), BF16),
            vmem((GROUPS, VOX, KG, PB), BF16),
            vmem((VIEWS, VOX, 2 * PB), BF16),
            vmem((VIEWS, HALF, 2 * PB), F32),
            vmem((VIEWS, HALF, 2 * PB), F32),
            vmem((VIEWS, HALF, 2 * PB), F32),
            vmem((VIEWS, 4, 4, 16, PIX), F32),
            vmem((VIEWS, 2, 16, PIX), I32),
            vmem((VIEWS, 2, 16, PIX), I32),
            vmem((VIEWS, 2, 2, 16, PIX), I32),
            vmem((VIEWS, 2, 2, 16, PIX), I32),
            vmem((2, VIEWS, 2, 1, PB), F32),
            vmem((2, VIEWS, 2, 1, PB), F32),
            vmem((VIEWS, 16, PIX), F32),
            vmem((VIEWS, 3, 8, PIX), I32),
            vmem((VIEWS, 3, 8, PIX), I32),
            vmem((VIEWS, 3, 1, PB), F32),
            vmem((VIEWS, 3, 1, PB), F32),
            vmem((2, 64, PB), F32),
            vmem((PAIRS, 8, 2, 4, PB), I32),
            vmem((PAIRS, 8, 2, 4, PB), I32),
            vmem((PAIRS, 2, 8, 4, PB), I32),
            vmem((PAIRS, 1, PB), F32),
            vmem((PAIRS, 8, 1, PB), F32),
            vmem((PAIRS, 2, 8, 1, PB), F32),
            vmem((32, 2 * PB), F32),
            vmem((8 * EBINS, len(MIX_ATT) * 32), BF16),
            vmem((64, 256), BF16),
            vmem((2, 32, 2 * PB), F32),
            vmem((2, 32, 2 * PB), F32),
            vmem((8, CBINS * OPITCH, PB), F32),
            dma((GROUPS + 1,)),
            dma, dma((PAIRS,)),
            dma, dma((PAIRS,)),
            dma, dma((PAIRS,)),
            dma, dma((PAIRS,)), dma((PAIRS,)),
            dma, dma((PAIRS,)),
            dma, dma((PAIRS,)),
            dma, dma((PAIRS,)),
            dma, dma((PAIRS,)),
            dma, dma((PAIRS,)),
            dma, dma((PAIRS,)),
            pltpu.SemaphoreType.REGULAR,
        ],
        compiler_params=pltpu.CompilerParams(
            collective_id=0, has_side_effects=True, vmem_limit_bytes=56 * 2**20
        ),
    )(
        volume.reshape(SLICES, VOX),
        system.reshape(VOX, KT, PB),
        geometry.T,
        attenuation,
        response,
        crosstalk,
    )


def solution(mesh):
    in_specs = (P("mat", None, "tile", None), P("tile", None, None, None), P(), P(), P(), P())
    out_specs = P(None, ("mat", "tile"), None, None)
    return jax.shard_map(
        per_device, mesh=mesh, in_specs=in_specs, out_specs=out_specs, check_vma=False
    )
```
